32 devices in a mesh: seq: 8 (over y, x, core), text: 4 (over z).
Axes of the slice: x: 2, y: 2, z: 4, core: 2. Of those that a mesh axis runs over, the one named last changes fastest.
Arguments:
- frames: bfloat16 [32768, 768], P(('seq', 'text')), may hold values from -6 to 6
- text_states: bfloat16 [48, 256, 1024], P('seq', 'text'), may hold values from -6 to 6
- timestep: bfloat16 [48, 768], P('seq'), may hold values from -6 to 6
- frame_lengths: int32 [8, 6], P('seq'), may hold values from 1 to 1000, 4096 in all within a row
- text_lengths: int32 [48], P('seq'), may hold values from 77 to 256
- cond_weight: bfloat16 [768, 4608], P('seq'), may hold values from -0.21875 to 0.21875
- cond_bias: bfloat16 [4608], P('seq'), may hold values from -3 to 3
- joint_weight: bfloat16 [768, 2304], P('seq'), may hold values from -0.21875 to 0.21875
- self_output: bfloat16 [768, 768], P('seq'), may hold values from -4 to 4
- query_weight: bfloat16 [768, 768], P('seq'), may hold values from -0.21875 to 0.21875
- text_weight: bfloat16 [1024, 1536], P('seq'), may hold values from -0.1875 to 0.1875
- cross_output: bfloat16 [768, 768], P('seq'), may hold values from -3 to 3
- up_weight: bfloat16 [768, 3072], P('seq'), may hold values from -0.21875 to 0.21875
- up_bias: bfloat16 [3072], P('seq'), may hold values from -3 to 3
- down_weight: bfloat16 [3072, 768], P('seq'), may hold values from -0.109375 to 0.109375
- down_bias: bfloat16 [768], P('seq'), may hold values from -3 to 3
- cotangent: bfloat16 [32768, 768], P(('seq', 'text')), may hold values from -6 to 6
Outputs:
- result: bfloat16 [32768, 768], P(('seq', 'text'))
- grad_frames: float32 [32768, 768], P(('seq', 'text'))
- grad_text: float32 [48, 256, 1024], P('seq', 'text')
- grad_cond_weight: float32 [768, 4608], P('seq')
- grad_cond_bias: float32 [4608], P('seq')
- grad_joint_weight: float32 [768, 2304], P('seq')
- grad_self_output: float32 [768, 768], P('seq')
- grad_query_weight: float32 [768, 768], P('seq')
- grad_text_weight: float32 [1024, 1536], P('seq')
- grad_cross_output: float32 [768, 768], P('seq')
- grad_up_weight: float32 [768, 3072], P('seq')
- grad_up_bias: float32 [3072], P('seq')
- grad_down_weight: float32 [3072, 768], P('seq')
- grad_down_bias: float32 [768], P('seq')
The draws below stay inside these ranges and needn't reach their ends.
Inputs may be any that keep to these rules, and one draw needn't show every extreme that they name: `frame_lengths`: row g gives the frame counts of the 6 items of group g in the order of their frames and sums to 4096; some item has exactly 1000 frames.
All inputs are finite; a program needn't handle non-finite values.
Results may differ from the reference program's by a relative error of at most 0.024.
The reference program's roundings to bfloat16 on the way count: a program that leaves them out, or rounds other values in their place, can miss the bound.
Values may be sent and summed in bfloat16 or wider, within the bound.
A program may use at most 320 MiB of HBM per device.

```python
import math
import jax
import jax.numpy as jnp
import numpy as np
from jax import lax

D = 768
HEADS = 12
HEAD_DIM = 64
FF = 3072
DT = 1024
ITEM_MAX = 1000
TLEN = 256
TXT_MIN = 77
GROUPS = 8
FRAMES_GRP = 4096
ITEMS_GRP = 6
ITEMS = 48
FRAMES = 32768


def place_ends(entries, stream_key, low, top_value):
    longest = entries.shape.index(max(entries.shape))
    spots = []
    for shift in (0, 1):
        where = [jax.random.randint(jax.random.fold_in(stream_key, axis), (), 0, length) for axis, length in enumerate(entries.shape)]
        where[longest] = (where[longest] + shift) % entries.shape[longest]
        spots.append(tuple(where))
    return entries.at[spots[0]].set(low).at[spots[1]].set(top_value)


def levels(own_key, extent, shards, least, largest):
    loudness = 1.0
    for axis_at, blocks in shards:
        heights = jax.random.uniform(jax.random.fold_in(jax.random.fold_in(own_key, 6), axis_at), (blocks,), jnp.float32, least / len(shards), largest / len(shards))
        loudness = loudness * jnp.repeat(jnp.exp(heights), extent[axis_at] // blocks).reshape((-1,) + (1,) * (len(extent) - 1 - axis_at))
    return loudness


def length_profile(number_of, total, limit, slope):
    loads = [(1 << 20) // math.isqrt(grade ** slope) + 1 for grade in range(2, number_of + 1)]
    rest, counts = total - limit - (number_of - 1), [1] * (number_of - 1)
    while rest > 0:
        candidates = [i for i in range(number_of - 1) if counts[i] < limit]
        whole, remaining = sum([loads[i] for i in candidates]), rest
        for i in candidates:
            addition = min(limit - counts[i], max(1, remaining * loads[i] // whole), rest)
            counts[i] = counts[i] + addition
            rest = rest - addition
    return np.array([limit] + counts)


def uneven(own_key, amount, total, bound, skew):
    if amount == 2:
        one = jax.random.randint(own_key, (), max(1, total - bound), min(bound, total - 1) + 1)
        return jnp.stack([one, total - one])
    lengths = jnp.asarray(length_profile(amount, total, bound, skew), jnp.int32)
    couples = (amount - 1) // 2
    source_of, receiver = lengths[1:1 + 2 * couples:2], lengths[2:2 + 2 * couples:2]
    room = jnp.minimum(source_of - 1, bound - receiver)
    shifted = jax.random.randint(jax.random.fold_in(own_key, 1), (couples,), 0, 1 << 20) % (room + 1)
    lengths = lengths.at[1:1 + 2 * couples:2].set(source_of - shifted).at[2:2 + 2 * couples:2].set(receiver + shifted)
    return lengths[jax.random.permutation(jax.random.fold_in(own_key, 2), amount)]


def normal_values(key, shape, width, most, shards=(), kind=jnp.bfloat16):
    loudness = levels(key, shape, shards, -0.22, 0.18) if shards else 1.0
    entries = jax.random.normal(key, shape, jnp.float32) * width * loudness
    return jnp.minimum(jnp.maximum(entries, -most), most).astype(kind)


def setup_inputs(seed: int = 0) -> dict:
    key_list = jax.random.split(jax.random.key(seed), 18)
    return {
        "frames": normal_values(key_list[0], (FRAMES, D), 1.0, 6.0, ((0, 32),)),
        "text_states": normal_values(key_list[1], (ITEMS, TLEN, DT), 1.0, 6.0, ((0, 8), (1, 4))),
        "timestep": normal_values(key_list[2], (ITEMS, D), 1.0, 6.0, ((0, 8),)),
        "frame_lengths": jax.vmap(lambda own: uneven(own, ITEMS_GRP, FRAMES_GRP, ITEM_MAX, 2))(jax.random.split(key_list[3], GROUPS)).reshape((GROUPS, ITEMS_GRP)).astype(jnp.int32),
        "text_lengths": place_ends(jax.random.randint(key_list[4], (ITEMS,), TXT_MIN, TLEN + 1), jax.random.fold_in(key_list[4], 1), TXT_MIN, TLEN).astype(jnp.int32),
        "cond_weight": normal_values(key_list[5], (D, 6 * D), D ** -0.5, 0.21875, ((0, 8),)),
        "cond_bias": normal_values(key_list[6], (6 * D,), 0.5, 3.0, ((0, 8),)),
        "joint_weight": normal_values(key_list[7], (D, 3 * D), D ** -0.5, 0.21875, ((0, 8),)),
        "self_output": normal_values(key_list[8], (D, D), 2 ** -0.5, 4.0, ((0, 8),)),
        "query_weight": normal_values(key_list[9], (D, D), D ** -0.5, 0.21875, ((0, 8),)),
        "text_weight": normal_values(key_list[10], (DT, 2 * D), DT ** -0.5, 0.1875, ((0, 8),)),
        "cross_output": normal_values(key_list[11], (D, D), 4 ** -0.5, 3.0, ((0, 8),)),
        "up_weight": normal_values(key_list[12], (D, FF), D ** -0.5, 0.21875, ((0, 8),)),
        "up_bias": normal_values(key_list[13], (FF,), 0.5, 3.0, ((0, 8),)),
        "down_weight": normal_values(key_list[14], (FF, D), FF ** -0.5, 0.109375, ((0, 8),)),
        "down_bias": normal_values(key_list[15], (D,), 0.5, 3.0, ((0, 8),)),
        "cotangent": normal_values(key_list[16], (FRAMES, D), 1.0, 6.0, ((0, 32),)),
    }


@jax.custom_vjp
def low(v):
    return lax.optimization_barrier(v.astype(jnp.bfloat16)).astype(jnp.float32)

@jax.custom_vjp
def low_back(v):
    return v

def low_keep(v):
    return (low(v), None)

def low_pass(kept, grad):
    return (grad,)

def back_keep(v):
    return (v, None)

def back_low(kept, grad):
    return (low(grad),)
low.defvjp(low_keep, low_pass)
low_back.defvjp(back_keep, back_low)
EPSILON = 1e-06
NEGATIVE = -1e+30

def matmul(left, right):
    return jnp.dot(left, right, precision=lax.Precision.HIGHEST)

def layer_norm(values):
    centre = values - lax.optimization_barrier(jnp.mean(values, axis=-1, keepdims=True))
    return centre * lax.rsqrt(lax.optimization_barrier(jnp.mean(centre * centre, axis=-1, keepdims=True)) + EPSILON)

def split_heads(matrix):
    return matrix.reshape(matrix.shape[0], HEADS, HEAD_DIM).transpose(1, 0, 2)

def join_heads(stacked):
    return stacked.transpose(1, 0, 2).reshape(stacked.shape[1], HEADS * HEAD_DIM)

def attend(queries, keys, values, allowed):
    factor = HEAD_DIM ** (-0.5)

    def one_head(pieces):
        query, key, value = pieces
        scores = low_back(matmul(query, key.T) * factor)
        weights = low(jax.nn.softmax(jnp.where(allowed, scores, NEGATIVE), axis=-1))
        return matmul(weights, value)
    stacked = lax.map(jax.checkpoint(one_head), (split_heads(queries), split_heads(keys), split_heads(values)))
    return join_heads(stacked)

def group_layer(weights, frame_part, text_part, cond_part, length_part, limit_part):
    cond_weight, cond_bias, joint_weight, self_output, query_weight, text_weight, cross_output, up_weight, up_bias, down_weight, down_bias = weights
    ends = jnp.cumsum(length_part).astype(jnp.int32)
    places = jnp.arange(FRAMES_GRP, dtype=jnp.int32)
    owner = lax.optimization_barrier(jnp.sum((places[:, None] >= ends[None, :]).astype(jnp.int32), axis=1))
    select = (owner[:, None] == jnp.arange(ITEMS_GRP, dtype=jnp.int32)[None, :]).astype(jnp.float32)
    modulation = matmul(low(jax.nn.silu(cond_part)), cond_weight) + cond_bias
    per_frame = matmul(select, modulation)
    shift_one, scale_one, gate_one, shift_two, scale_two, gate_two = jnp.split(per_frame, 6, axis=1)
    normed_one = low(layer_norm(frame_part) * (1.0 + scale_one) + shift_one)
    triple = low(low_back(matmul(normed_one, joint_weight)))
    queries, keys, values = jnp.split(triple, 3, axis=1)
    same_item = owner[:, None] == owner[None, :]
    mixed = low(low_back(attend(queries, keys, values, same_item)))
    after_self = frame_part + gate_one * low_back(matmul(mixed, self_output))
    cross_query = low(low_back(matmul(low(layer_norm(after_self)), query_weight)))
    flat_text = text_part.reshape(ITEMS_GRP * TLEN, DT)
    text_kv = low(low_back(matmul(flat_text, text_weight)))
    text_keys, text_values = jnp.split(text_kv, 2, axis=1)
    token_index = jnp.arange(ITEMS_GRP * TLEN, dtype=jnp.int32)
    token_item = token_index // TLEN
    token_place = token_index % TLEN
    valid = token_place < limit_part[token_item]
    cross_allowed = (owner[:, None] == token_item[None, :]) & valid[None, :]
    cross_mixed = low(low_back(attend(cross_query, text_keys, text_values, cross_allowed)))
    after_cross = after_self + low_back(matmul(cross_mixed, cross_output))
    normed_three = low(layer_norm(after_cross) * (1.0 + scale_two) + shift_two)
    hidden = low_back(matmul(normed_three, up_weight) + up_bias)
    activated = low(jax.nn.gelu(hidden, approximate=True))
    return after_cross + gate_two * low_back(matmul(activated, down_weight) + down_bias)

def reference(frames, text_states, timestep, frame_lengths, text_lengths, cond_weight, cond_bias, joint_weight, self_output, query_weight, text_weight, cross_output, up_weight, up_bias, down_weight, down_bias, cotangent):
    params = tuple((entry.astype(jnp.float32) for entry in (cond_weight, cond_bias, joint_weight, self_output, query_weight, text_weight, cross_output, up_weight, up_bias, down_weight, down_bias)))
    frame_groups = frames.astype(jnp.float32).reshape(GROUPS, FRAMES_GRP, D)
    text_groups = text_states.astype(jnp.float32).reshape(GROUPS, ITEMS_GRP, TLEN, DT)
    cond_groups = timestep.astype(jnp.float32).reshape(GROUPS, ITEMS_GRP, D)
    limit_groups = text_lengths.reshape(GROUPS, ITEMS_GRP)

    def forward(weights, frame_all, text_all):

        def group_step(carry, pieces):
            frame_part, text_part, cond_part, length_part, limit_part = pieces
            output = jax.checkpoint(group_layer)(weights, frame_part, text_part, cond_part, length_part, limit_part)
            return (carry, output)
        return lax.scan(group_step, jnp.zeros((), jnp.float32), (frame_all, text_all, cond_groups, frame_lengths, limit_groups))[1]
    outputs, pullback = jax.vjp(forward, params, frame_groups, text_groups)
    grad_params, grad_frames, grad_text = pullback(cotangent.astype(jnp.float32).reshape(GROUPS, FRAMES_GRP, D))
    grad_cond_weight, grad_cond_bias, grad_joint, grad_self_output, grad_query_weight, grad_text_weight, grad_cross_output, grad_up, grad_up_bias, grad_down, grad_down_bias = grad_params
    return (outputs.reshape(FRAMES, D).astype(jnp.bfloat16), grad_frames.reshape(FRAMES, D), grad_text.reshape(ITEMS, TLEN, DT), grad_cond_weight, grad_cond_bias, grad_joint, grad_self_output, grad_query_weight, grad_text_weight, grad_cross_output, grad_up, grad_up_bias, grad_down, grad_down_bias)
```

```python
import functools

import jax
import jax.numpy as jnp
from jax import lax
from jax.experimental import pallas as pl
from jax.experimental.pallas import tpu as pltpu
from jax.sharding import PartitionSpec as P

HEADS = 12
HEAD_DIM = 64
PAIR = 2 * HEAD_DIM
EPSILON = 1e-06
BLOCK_Q = 256
BLOCK_K = 256
PENALTY = -1e30
VMEM_LIMIT = 60 * 1024 * 1024

BF16 = jnp.bfloat16
F32 = jnp.float32


def contract(left, right, dims):
    return lax.dot_general(left, right, (dims, ((), ())), preferred_element_type=F32)


def product(left, right):
    return contract(left, right, ((1,), (0,)))


def contract_first(left, right):
    return contract(left, right, ((0,), (0,)))


def contract_last(left, right):
    return contract(left, right, ((1,), (1,)))


def halves():
    lane = lax.broadcasted_iota(jnp.int32, (1, PAIR), 1)
    low = (lane < HEAD_DIM).astype(F32).astype(BF16)
    return low, (lane >= HEAD_DIM).astype(F32).astype(BF16)


def rows_of(block, size):
    return pl.ds(pl.multiple_of(block * size, size), size)


def forward_kernel(bounds, q_ref, k_ref, v_ref, qt_ref, kt_ref, o_ref, lse_ref, ka_ref, vt_ref):
    low, high = halves()
    key_blocks = k_ref.shape[0] // BLOCK_K

    @pl.loop(0, key_blocks)
    def _(b):
        rows = rows_of(b, BLOCK_K)
        keys, tags = k_ref[rows, :], kt_ref[rows, :]
        ka_ref[0, rows, :] = keys * low + tags * high
        ka_ref[1, rows, :] = keys * high + tags * low
        vt_ref[:, rows] = v_ref[rows, :].astype(F32).T.astype(BF16)

    @pl.loop(0, q_ref.shape[0] // BLOCK_Q)
    def _(i):
        mine = rows_of(i, BLOCK_Q)
        queries, tags = q_ref[mine, :], qt_ref[mine, :]
        tagged = (queries * low + tags * high, queries * high + tags * low)

        def step(b, carry):
            rows = rows_of(b, BLOCK_K)
            following = []
            for h in range(2):
                peak, total, acc = carry[h]
                scores = contract_last(ka_ref[h, rows, :], tagged[h])
                top = jnp.maximum(peak, jnp.max(scores, axis=0, keepdims=True))
                fade = jnp.exp(peak - top)
                expos = jnp.exp(scores - top)
                total = total * fade + jnp.sum(expos, axis=0, keepdims=True)
                values = vt_ref[h * HEAD_DIM : (h + 1) * HEAD_DIM, rows]
                acc = acc * fade + product(values, expos.astype(BF16))
                following.append((top, total, acc))
            return tuple(following)

        start = (
            jnp.full((1, BLOCK_Q), 2 * PENALTY, F32),
            jnp.zeros((1, BLOCK_Q), F32),
            jnp.zeros((HEAD_DIM, BLOCK_Q), F32),
        )
        ended = lax.fori_loop(bounds[0, i], bounds[1, i], step, (start, start))
        outs = jnp.concatenate([acc / total for _, total, acc in ended], axis=0)
        o_ref[mine, :] = outs.T.astype(BF16)
        for h in range(2):
            lse_ref[0, h : h + 1, mine] = ended[h][0] + jnp.log(ended[h][1])


def backward_kernel(
    bounds, q_ref, k_ref, v_ref, g_ref, qt_ref, kt_ref, lse_ref, delta_ref,
    dq_ref, dk_ref, dv_ref, ka_ref, kt_s, dqt, dk_acc, dv_acc,
):
    low, high = halves()
    key_blocks = k_ref.shape[0] // BLOCK_K

    @pl.loop(0, key_blocks)
    def _(b):
        rows = rows_of(b, BLOCK_K)
        keys, tags = k_ref[rows, :], kt_ref[rows, :]
        ka_ref[0, rows, :] = keys * low + tags * high
        ka_ref[1, rows, :] = keys * high + tags * low
        kt_s[:, rows] = keys.astype(F32).T.astype(BF16)
        dk_acc[rows, :] = jnp.zeros((BLOCK_K, PAIR), F32)
        dv_acc[rows, :] = jnp.zeros((BLOCK_K, PAIR), F32)

    @pl.loop(0, q_ref.shape[0] // BLOCK_Q)
    def _(i):
        mine = rows_of(i, BLOCK_Q)
        queries, tags, grads = q_ref[mine, :], qt_ref[mine, :], g_ref[mine, :]
        plain = (queries * low, queries * high)
        tagged = (plain[0] + tags * high, plain[1] + tags * low)
        split = (grads * low, grads * high)
        q_cat = jnp.concatenate(plain, axis=0)
        g_cat = jnp.concatenate(split, axis=0)
        lses = [lse_ref[0, h : h + 1, mine] for h in range(2)]
        deltas = [delta_ref[0, h : h + 1, mine] for h in range(2)]
        dqt[...] = jnp.zeros(dqt.shape, F32)

        @pl.loop(bounds[0, i], bounds[1, i])
        def _(b):
            rows = rows_of(b, BLOCK_K)
            values = v_ref[rows, :]
            weights, slopes = [], []
            for h in range(2):
                scores = contract_last(ka_ref[h, rows, :], tagged[h])
                expos = jnp.exp(scores - lses[h])
                pull = contract_last(values, split[h])
                slope = (expos * (pull - deltas[h])).astype(BF16)
                weights.append(expos.astype(BF16))
                slopes.append(slope)
                part = slice(h * HEAD_DIM, (h + 1) * HEAD_DIM)
                dqt[part, :] += product(kt_s[part, rows], slope)
            dv_acc[rows, :] += product(jnp.concatenate(weights, axis=1), g_cat)
            dk_acc[rows, :] += product(jnp.concatenate(slopes, axis=1), q_cat)

        dq_ref[mine, :] = (dqt[...] * HEAD_DIM ** (-0.5)).T.astype(BF16)

    @pl.loop(0, key_blocks)
    def _(b):
        rows = rows_of(b, BLOCK_K)
        dk_ref[rows, :] = dk_acc[rows, :].astype(BF16)
        dv_ref[rows, :] = dv_acc[rows, :].astype(BF16)


def column(rows):
    return pl.BlockSpec((rows, PAIR), lambda j, *_: (0, j))


def shared(rows):
    return pl.BlockSpec((rows, PAIR), lambda j, *_: (0, 0))


def stat(rows):
    return pl.BlockSpec((1, 8, rows), lambda j, *_: (j, 0, 0))


def cost(rows, keys, matmuls):
    return pl.CostEstimate(
        flops=matmuls * rows * keys * HEADS * HEAD_DIM, bytes_accessed=8 * (rows + keys) * HEADS * HEAD_DIM,
        transcendentals=rows * keys * HEADS // 2,
    )


def attend(bounds, query, key, value, query_tags, key_tags):
    rows, width = query.shape
    keys = key.shape[0]
    return pl.pallas_call(
        forward_kernel,
        out_shape=(
            jax.ShapeDtypeStruct((rows, width), BF16),
            jax.ShapeDtypeStruct((width // PAIR, 8, rows), F32),
        ),
        grid_spec=pltpu.PrefetchScalarGridSpec(
            num_scalar_prefetch=1,
            grid=(width // PAIR,),
            in_specs=[column(rows), column(keys), column(keys), shared(rows), shared(keys)],
            out_specs=[column(rows), stat(rows)],
            scratch_shapes=[pltpu.VMEM((2, keys, PAIR), BF16), pltpu.VMEM((PAIR, keys), BF16)],
        ),
        compiler_params=pltpu.CompilerParams(vmem_limit_bytes=VMEM_LIMIT),
        cost_estimate=cost(rows, keys, 4),
        name="attend",
    )(bounds, query, key, value, query_tags, key_tags)


def attend_back(bounds, query, key, value, grad, query_tags, key_tags, lse, delta):
    rows, width = query.shape
    keys = key.shape[0]
    return pl.pallas_call(
        backward_kernel,
        out_shape=(
            jax.ShapeDtypeStruct((rows, width), BF16),
            jax.ShapeDtypeStruct((keys, width), BF16),
            jax.ShapeDtypeStruct((keys, width), BF16),
        ),
        grid_spec=pltpu.PrefetchScalarGridSpec(
            num_scalar_prefetch=1,
            grid=(width // PAIR,),
            in_specs=[
                column(rows), column(keys), column(keys), column(rows), shared(rows), shared(keys),
                stat(rows), stat(rows),
            ],
            out_specs=[column(rows), column(keys), column(keys)],
            scratch_shapes=[
                pltpu.VMEM((2, keys, PAIR), BF16),
                pltpu.VMEM((PAIR, keys), BF16),
                pltpu.VMEM((PAIR, BLOCK_Q), F32),
                pltpu.VMEM((keys, PAIR), F32),
                pltpu.VMEM((keys, PAIR), F32),
            ],
        ),
        compiler_params=pltpu.CompilerParams(vmem_limit_bytes=VMEM_LIMIT),
        cost_estimate=cost(rows, keys, 10),
        name="attend_back",
    )(bounds, query, key, value, grad, query_tags, key_tags, lse, delta)


def head_stats(grad, out):
    rows, width = out.shape
    sums = jnp.sum((grad.astype(F32) * out.astype(F32)).reshape(rows, HEADS, HEAD_DIM), axis=2)
    pairs = sums.T.reshape(HEADS // 2, 2, rows)
    return jnp.pad(pairs, ((0, 0), (0, 6), (0, 0)))


def tag_lanes(kind, items):
    lane = jnp.arange(PAIR, dtype=jnp.int32)[None, :] % HEAD_DIM
    kind = jnp.where(kind < 0, items, kind)[:, None]
    key_tags = (lane == kind).astype(BF16)
    query_tags = jnp.where((lane != kind) & (lane <= items), PENALTY, 0.0).astype(BF16)
    return query_tags, key_tags


def layer_norm(values):
    centre = values - jnp.mean(values, axis=-1, keepdims=True)
    return centre * lax.rsqrt(jnp.mean(centre * centre, axis=-1, keepdims=True) + EPSILON)


def modulate(values, shift, scale):
    return layer_norm(values) * (1.0 + scale) + shift


def of_owner(owner, table):
    chosen = jnp.broadcast_to(table[0][None, :], (owner.shape[0], table.shape[1]))
    for item in range(1, table.shape[0]):
        chosen = jnp.where((owner == item)[:, None], table[item][None, :], chosen)
    return chosen


def per_item(owner, items, values):
    select = (jnp.arange(items, dtype=jnp.int32)[:, None] == owner[None, :]).astype(BF16)
    coarse = lax.reduce_precision(values, 8, 7)
    fine = lax.reduce_precision(values - coarse, 8, 7)
    return product(select, coarse.astype(BF16)) + product(select, fine.astype(BF16))


def shifted(x, axis, by):
    size = lax.axis_size(axis)
    return lax.ppermute(x, axis, [(i, (i + by) % size) for i in range(size)])


def neighbour(x, axis, by):
    size = lax.axis_size(axis)
    return lax.ppermute(x, axis, [(i, i + by) for i in range(size) if 0 <= i + by < size])


def scattered(grads, axis):
    return lax.psum_scatter(grads.astype(BF16), axis, scatter_dimension=0, tiled=True)


def body(
    frames, text_states, timestep, frame_lengths, text_lengths,
    cond_weight, cond_bias, joint_weight, self_output, query_weight, text_weight, cross_output,
    up_weight, up_bias, down_weight, down_bias, cotangent,
):
    rows, width = frames.shape
    parts, position = lax.axis_size("text"), lax.axis_index("text")
    groups, group = lax.axis_size("seq"), lax.axis_index("seq")
    items, tokens, text_width = text_states.shape
    mod_width = cond_weight.shape[1]

    small = jnp.concatenate([timestep.reshape(-1), cond_bias, up_bias, down_bias])
    small_all = lax.all_gather(small, "seq", axis=0)
    joint_full = lax.all_gather(joint_weight, "seq", axis=0, tiled=True)
    outer_full = lax.all_gather(
        jnp.concatenate([self_output, query_weight, cross_output], axis=1), "seq", axis=0, tiled=True
    )
    text_full = lax.all_gather(text_weight, "seq", axis=0, tiled=True)
    up_full = lax.all_gather(up_weight, "seq", axis=0, tiled=True)
    down_full = lax.all_gather(down_weight, "seq", axis=0, tiled=True)
    before = neighbour(frames, "text", 1)
    after = neighbour(frames, "text", -1)
    flat_text = text_states.reshape(items * tokens, text_width)
    text_parts = [text_states] + [shifted(text_states, "text", k) for k in range(1, parts)]

    cut = timestep.size
    steps_all = small_all[:, :cut].reshape(groups * items, width)
    cond_bias_full = small_all[:, cut : cut + cond_bias.size].reshape(-1).astype(F32)
    cut += cond_bias.size
    up_bias_full = small_all[:, cut : cut + up_bias.size].reshape(-1).astype(F32)
    cut += up_bias.size
    down_bias_full = small_all[:, cut:].reshape(-1).astype(F32)

    silu_all = jax.nn.silu(steps_all.astype(F32)).astype(BF16)
    slab = cond_weight.shape[0]
    silu_mine = lax.dynamic_slice_in_dim(silu_all, group * slab, slab, axis=1)
    modulation = (
        lax.psum_scatter(product(silu_mine, cond_weight), "seq", scatter_dimension=0, tiled=True)
        + cond_bias_full
    )

    ends = jnp.cumsum(frame_lengths[0])
    starts = ends - frame_lengths[0]

    def item_of(places):
        inside = (places >= 0) & (places < rows * parts)
        found = jnp.sum((places[:, None] >= ends[None, :]).astype(jnp.int32), axis=1)
        return jnp.where(inside, found, -1)

    origin = (position - 1) * rows
    window_item = item_of(origin + jnp.arange(3 * rows, dtype=jnp.int32))
    own_item = window_item[rows : 2 * rows]
    token_index = jnp.arange(items * parts * tokens, dtype=jnp.int32)
    token_item = token_index // (parts * tokens)
    in_item = token_index % (parts * tokens)
    token_place = ((position - in_item // tokens) % parts) * tokens + in_item % tokens
    token_kind = jnp.where(token_place < text_lengths[token_item], token_item, -1)
    query_tags, _ = tag_lanes(own_item, items)
    _, window_tags = tag_lanes(window_item, items)
    _, token_tags = tag_lanes(token_kind, items)
    firsts = own_item[:: BLOCK_Q]
    lasts = own_item[BLOCK_Q - 1 :: BLOCK_Q]
    self_bounds = jnp.stack(
        [(starts[firsts] - origin) // BLOCK_K, (ends[lasts] - origin + BLOCK_K - 1) // BLOCK_K]
    )
    per_text = parts * tokens // BLOCK_K
    cross_bounds = jnp.stack([firsts * per_text, (lasts + 1) * per_text])

    source = jnp.concatenate([before, frames, after], axis=0).astype(F32)
    own = slice(rows, 2 * rows)
    blocks = [modulation[:, i * width : (i + 1) * width] for i in range(6)]
    shift_one = of_owner(window_item, blocks[0])
    scale_one = of_owner(window_item, blocks[1])
    gate_one, shift_two, scale_two, gate_two = [of_owner(own_item, table) for table in blocks[2:]]
    normed_one = modulate(source, shift_one, scale_one).astype(BF16)
    factor = HEAD_DIM ** (-0.5)
    query = product(normed_one[own], joint_full[:, :width]).astype(BF16) * BF16(factor)
    keyvalue = product(normed_one, joint_full[:, width:]).astype(BF16)
    key, value = keyvalue[:, :width], keyvalue[:, width:]
    mixed, self_lse = attend(self_bounds, query, key, value, query_tags, window_tags)
    output_full = outer_full[:, :width]
    query_full = outer_full[:, width : 2 * width]
    cross_full = outer_full[:, 2 * width :]
    self_branch = product(mixed, output_full)
    after_self = source[own] + gate_one * self_branch
    normed_two = layer_norm(after_self).astype(BF16)
    cross_query = product(normed_two, query_full).astype(BF16) * BF16(factor)
    text_all = jnp.concatenate(text_parts, axis=1).reshape(items * parts * tokens, text_width)
    text_kv = product(text_all, text_full).astype(BF16)
    text_key, text_value = text_kv[:, :width], text_kv[:, width:]
    cross_mixed, cross_lse = attend(
        cross_bounds, cross_query, text_key, text_value, query_tags, token_tags
    )
    after_cross = after_self + product(cross_mixed, cross_full)
    normed_three = modulate(after_cross, shift_two, scale_two).astype(BF16)
    hidden = product(normed_three, up_full) + up_bias_full
    activated = jax.nn.gelu(hidden, approximate=True).astype(BF16)
    mlp_branch = product(activated, down_full) + down_bias_full
    result = (after_cross + gate_two * mlp_branch).astype(BF16)

    upstream = cotangent.astype(F32)
    grad_gate_two = upstream * mlp_branch
    grad_branch = (gate_two * upstream).astype(BF16)
    share_down = scattered(contract_first(activated, grad_branch), "seq")
    grad_down_bias = jnp.sum(grad_branch.astype(F32), axis=0)
    grad_activated = contract_last(grad_branch, down_full)
    _, gelu_pull = jax.vjp(lambda entry: jax.nn.gelu(entry, approximate=True), hidden)
    grad_hidden = gelu_pull(grad_activated)[0].astype(BF16)
    share_up = scattered(contract_first(normed_three, grad_hidden), "seq")
    grad_up_bias = jnp.sum(grad_hidden.astype(F32), axis=0)
    grad_normed_three = contract_last(grad_hidden, up_full)
    _, third_pull = jax.vjp(modulate, after_cross, shift_two, scale_two)
    grad_after_cross, grad_shift_two, grad_scale_two = third_pull(grad_normed_three)
    grad_after_cross = grad_after_cross + upstream
    grad_cross_branch = grad_after_cross.astype(BF16)
    grad_cross_output = contract_first(cross_mixed, grad_cross_branch)
    grad_cross_mixed = contract_last(grad_cross_branch, cross_full).astype(BF16)
    grad_cross_query, grad_text_key, grad_text_value = attend_back(
        cross_bounds, cross_query, text_key, text_value, grad_cross_mixed, query_tags, token_tags,
        cross_lse, head_stats(grad_cross_mixed, cross_mixed),
    )
    grad_text_all = jnp.concatenate([grad_text_key, grad_text_value], axis=1)
    grad_text_all = grad_text_all.reshape(items, parts, tokens, 2 * width)
    grad_text_kv = grad_text_all[:, 0].astype(F32)
    for k in range(1, parts):
        grad_text_kv = grad_text_kv + shifted(grad_text_all[:, k], "text", -k).astype(F32)
    grad_text_kv = grad_text_kv.astype(BF16).reshape(items * tokens, 2 * width)
    share_text = scattered(contract_first(flat_text, grad_text_kv), "seq")
    grad_text = contract_last(grad_text_kv, text_full).reshape(text_states.shape)
    grad_query_weight = contract_first(normed_two, grad_cross_query)
    grad_normed_two = contract_last(grad_cross_query, query_full)
    _, norm_pull = jax.vjp(layer_norm, after_self)
    grad_after_self = grad_after_cross + norm_pull(grad_normed_two)[0]
    grad_gate_one = grad_after_self * self_branch
    grad_self_branch = (gate_one * grad_after_self).astype(BF16)
    grad_self_output = contract_first(mixed, grad_self_branch)
    share_outer = scattered(
        jnp.concatenate([grad_self_output, grad_query_weight, grad_cross_output], axis=1), "seq"
    )
    grad_mixed = contract_last(grad_self_branch, output_full).astype(BF16)
    grad_query, grad_key, grad_value = attend_back(
        self_bounds, query, key, value, grad_mixed, query_tags, window_tags,
        self_lse, head_stats(grad_mixed, mixed),
    )
    grad_keyvalue = jnp.concatenate([grad_key, grad_value], axis=1)
    share_joint = scattered(
        jnp.concatenate(
            [contract_first(normed_one[own], grad_query), contract_first(normed_one, grad_keyvalue)],
            axis=1,
        ),
        "seq",
    )
    grad_normed_one = contract_last(grad_keyvalue, joint_full[:, width:])
    grad_normed_own = contract_last(grad_query, joint_full[:, :width])
    grad_normed_one = jnp.concatenate(
        [grad_normed_one[:rows], grad_normed_one[own] + grad_normed_own, grad_normed_one[2 * rows :]]
    )
    _, first_pull = jax.vjp(modulate, source, shift_one, scale_one)
    grad_source, grad_shift_one, grad_scale_one = first_pull(grad_normed_one)
    from_next = neighbour(grad_source[:rows].astype(BF16), "text", -1)
    from_previous = neighbour(grad_source[2 * rows :].astype(BF16), "text", 1)
    grad_frames = (
        grad_source[own] + grad_after_self + from_next.astype(F32) + from_previous.astype(F32)
    )
    late = per_item(window_item, items, jnp.concatenate([grad_shift_one, grad_scale_one], axis=1))
    early = per_item(
        own_item, items,
        jnp.concatenate([grad_gate_one, grad_shift_two, grad_scale_two, grad_gate_two], axis=1),
    )
    grad_modulation = jnp.concatenate([late, early], axis=1)
    sums = jnp.concatenate([grad_modulation.reshape(-1), grad_up_bias, grad_down_bias])
    sums_all = lax.all_gather(lax.psum(sums, "text"), "seq", axis=0)
    cut = items * mod_width
    grad_mod_all = sums_all[:, :cut].reshape(groups * items, mod_width)
    grad_cond_weight = lax.dot_general(
        silu_mine.astype(F32), grad_mod_all, (((0,), (0,)), ((), ())), precision=lax.Precision.HIGHEST
    )
    grad_cond_bias = jnp.sum(
        lax.dynamic_slice_in_dim(grad_mod_all, group * cond_bias.size, cond_bias.size, axis=1), axis=0
    )
    bias_sums = jnp.sum(sums_all[:, cut:], axis=0)
    share_up_bias = lax.dynamic_slice_in_dim(
        bias_sums[: up_bias.size * groups], group * up_bias.size, up_bias.size
    )
    share_down_bias = lax.dynamic_slice_in_dim(
        bias_sums[up_bias.size * groups :], group * down_bias.size, down_bias.size
    )
    shares = [
        lax.psum(share, "text").astype(F32)
        for share in (share_joint, share_outer, share_text, share_up, share_down)
    ]
    outer = shares[1]
    return (
        result, grad_frames, grad_text, grad_cond_weight, grad_cond_bias, shares[0],
        outer[:, :width], outer[:, width : 2 * width], shares[2], outer[:, 2 * width :],
        shares[3], share_up_bias, shares[4], share_down_bias,
    )


def solution(mesh):
    both, seq, flat = P(("seq", "text"), None), P("seq", None), P("seq")
    texts = P("seq", "text", None)
    return jax.shard_map(
        body,
        mesh=mesh,
        in_specs=(
            both, texts, seq, seq, flat, seq, flat, seq, seq, seq, seq, seq, seq, flat, seq, flat, both,
        ),
        out_specs=(
            both, both, texts, seq, flat, seq, seq, seq, seq, seq, seq, flat, seq, flat,
        ),
        check_vma=False,
    )
```

```python
import functools

import jax
import jax.numpy as jnp
from jax import lax
from jax.experimental import pallas as pl
from jax.experimental.pallas import tpu as pltpu
from jax.sharding import PartitionSpec as P

HEADS = 12
HEAD_DIM = 64
PAIR = 2 * HEAD_DIM
EPSILON = 1e-06
BLOCK_Q = 256
BLOCK_K = 256
PENALTY = -1e30
VMEM_LIMIT = 60 * 1024 * 1024

BF16 = jnp.bfloat16
F32 = jnp.float32


def contract(left, right, dims):
    return lax.dot_general(left, right, (dims, ((), ())), preferred_element_type=F32)


def product(left, right):
    return contract(left, right, ((1,), (0,)))


def contract_first(left, right):
    return contract(left, right, ((0,), (0,)))


def contract_last(left, right):
    return contract(left, right, ((1,), (1,)))


def halves():
    lane = lax.broadcasted_iota(jnp.int32, (1, PAIR), 1)
    low = (lane < HEAD_DIM).astype(F32).astype(BF16)
    return low, (lane >= HEAD_DIM).astype(F32).astype(BF16)


def rows_of(block, size):
    return pl.ds(pl.multiple_of(block * size, size), size)


def forward_kernel(bounds, q_ref, k_ref, v_ref, qt_ref, kt_ref, o_ref, lse_ref, ka_ref, vt_ref):
    low, high = halves()
    last_block = q_ref.shape[0] // BLOCK_Q - 1
    ones = jnp.ones((16, BLOCK_K), F32).astype(BF16)

    @pl.loop(bounds[0, 0], bounds[1, last_block])
    def _(b):
        rows = rows_of(b, BLOCK_K)
        keys, tags = k_ref[rows, :], kt_ref[rows, :]
        ka_ref[0, rows, :] = keys * low + tags * high
        ka_ref[1, rows, :] = keys * high + tags * low
        turned = v_ref[rows, :].astype(F32).T.astype(BF16)
        vt_ref[0, :HEAD_DIM, rows] = turned[:HEAD_DIM]
        vt_ref[1, :HEAD_DIM, rows] = turned[HEAD_DIM:]
        vt_ref[0, HEAD_DIM:, rows] = ones
        vt_ref[1, HEAD_DIM:, rows] = ones

    @pl.loop(0, q_ref.shape[0] // BLOCK_Q)
    def _(i):
        mine = rows_of(i, BLOCK_Q)
        queries, tags = q_ref[mine, :], qt_ref[mine, :]
        tagged = (queries * low + tags * high, queries * high + tags * low)
        first, last = bounds[0, i], bounds[1, i]

        def scored(b):
            return tuple(contract_last(ka_ref[h, rows_of(b, BLOCK_K), :], tagged[h]) for h in range(2))

        def step(b, carry):
            states, scores = carry
            later = scored(jnp.minimum(b + 1, last - 1))
            rows = rows_of(b, BLOCK_K)
            following = []
            for h in range(2):
                peak, acc = states[h]
                top = jnp.maximum(peak, jnp.max(scores[h], axis=0, keepdims=True))
                fade = jnp.exp(peak - top)
                expos = jnp.exp(scores[h] - top).astype(BF16)
                acc = acc * fade + product(vt_ref[h, :, rows], expos)
                following.append((top, acc))
            return tuple(following), later

        start = (jnp.full((1, BLOCK_Q), 2 * PENALTY, F32), jnp.zeros((HEAD_DIM + 16, BLOCK_Q), F32))
        ended, _ = lax.fori_loop(first, last, step, ((start, start), scored(first)))
        totals = [acc[HEAD_DIM : HEAD_DIM + 1] for _, acc in ended]
        outs = jnp.concatenate([acc[:HEAD_DIM] / total for total, (_, acc) in zip(totals, ended)], axis=0)
        o_ref[mine, :] = outs.T.astype(BF16)
        for h in range(2):
            lse_ref[0, h : h + 1, mine] = ended[h][0] + jnp.log(totals[h])

def backward_kernel(
    bounds, q_ref, k_ref, v_ref, g_ref, qt_ref, kt_ref, lse_ref, delta_ref,
    dq_ref, dk_ref, dv_ref, ka_ref, kt_s, dqt, dk_acc, dv_acc,
):
    low, high = halves()
    key_blocks = k_ref.shape[0] // BLOCK_K

    @pl.loop(0, key_blocks)
    def _(b):
        rows = rows_of(b, BLOCK_K)
        keys, tags = k_ref[rows, :], kt_ref[rows, :]
        ka_ref[0, rows, :] = keys * low + tags * high
        ka_ref[1, rows, :] = keys * high + tags * low
        kt_s[:, rows] = keys.astype(F32).T.astype(BF16)
        dk_acc[:, rows] = jnp.zeros((PAIR, BLOCK_K), F32)
        dv_acc[:, rows] = jnp.zeros((PAIR, BLOCK_K), F32)

    @pl.loop(0, q_ref.shape[0] // BLOCK_Q)
    def _(i):
        mine = rows_of(i, BLOCK_Q)
        queries, tags, grads = q_ref[mine, :], qt_ref[mine, :], g_ref[mine, :]
        tagged = (queries * low + tags * high, queries * high + tags * low)
        split = (grads * low, grads * high)
        q_turned = queries.astype(F32).T.astype(BF16)
        g_turned = grads.astype(F32).T.astype(BF16)
        lses = [lse_ref[0, h : h + 1, mine] for h in range(2)]
        deltas = [delta_ref[0, h : h + 1, mine] for h in range(2)]
        dqt[...] = jnp.zeros(dqt.shape, F32)
        first, last = bounds[0, i], bounds[1, i]

        @pl.loop(first, last)
        def _(b):
            rows = rows_of(b, BLOCK_K)
            values = v_ref[rows, :]
            for h in range(2):
                scores = contract_last(ka_ref[h, rows, :], tagged[h])
                pull = contract_last(values, split[h])
                expos = jnp.exp(scores - lses[h])
                slope = (expos * (pull - deltas[h])).astype(BF16)
                weight = expos.astype(BF16)
                part = slice(h * HEAD_DIM, (h + 1) * HEAD_DIM)
                dqt[part, :] += product(kt_s[part, rows], slope)
                dk_acc[part, rows] += contract_last(q_turned[part], slope)
                dv_acc[part, rows] += contract_last(g_turned[part], weight)

        dq_ref[mine, :] = (dqt[...] * HEAD_DIM ** (-0.5)).T.astype(BF16)

    @pl.loop(0, key_blocks)
    def _(b):
        rows = rows_of(b, BLOCK_K)
        dk_ref[rows, :] = dk_acc[:, rows].T.astype(BF16)
        dv_ref[rows, :] = dv_acc[:, rows].T.astype(BF16)

def column(rows):
    return pl.BlockSpec((rows, PAIR), lambda j, *_: (0, j))


def shared(rows):
    return pl.BlockSpec((rows, PAIR), lambda j, *_: (0, 0))


def stat(rows):
    return pl.BlockSpec((1, 8, rows), lambda j, *_: (j, 0, 0))


def cost(rows, keys, matmuls):
    return pl.CostEstimate(
        flops=matmuls * rows * keys * HEADS * HEAD_DIM, bytes_accessed=8 * (rows + keys) * HEADS * HEAD_DIM,
        transcendentals=rows * keys * HEADS // 2,
    )


def attend(bounds, query, key, value, query_tags, key_tags):
    rows, width = query.shape
    keys = key.shape[0]
    return pl.pallas_call(
        forward_kernel,
        out_shape=(
            jax.ShapeDtypeStruct((rows, width), BF16),
            jax.ShapeDtypeStruct((width // PAIR, 8, rows), F32),
        ),
        grid_spec=pltpu.PrefetchScalarGridSpec(
            num_scalar_prefetch=1,
            grid=(width // PAIR,),
            in_specs=[column(rows), column(keys), column(keys), shared(rows), shared(keys)],
            out_specs=[column(rows), stat(rows)],
            scratch_shapes=[
                pltpu.VMEM((2, keys, PAIR), BF16),
                pltpu.VMEM((2, HEAD_DIM + 16, keys), BF16),
            ],
        ),
        compiler_params=pltpu.CompilerParams(vmem_limit_bytes=VMEM_LIMIT),
        cost_estimate=cost(rows, keys, 4),
        name="attend",
    )(bounds, query, key, value, query_tags, key_tags)


def attend_back(bounds, query, key, value, grad, query_tags, key_tags, lse, delta):
    rows, width = query.shape
    keys = key.shape[0]
    return pl.pallas_call(
        backward_kernel,
        out_shape=(
            jax.ShapeDtypeStruct((rows, width), BF16),
            jax.ShapeDtypeStruct((keys, width), BF16),
            jax.ShapeDtypeStruct((keys, width), BF16),
        ),
        grid_spec=pltpu.PrefetchScalarGridSpec(
            num_scalar_prefetch=1,
            grid=(width // PAIR,),
            in_specs=[
                column(rows), column(keys), column(keys), column(rows), shared(rows), shared(keys),
                stat(rows), stat(rows),
            ],
            out_specs=[column(rows), column(keys), column(keys)],
            scratch_shapes=[
                pltpu.VMEM((2, keys, PAIR), BF16),
                pltpu.VMEM((PAIR, keys), BF16),
                pltpu.VMEM((PAIR, BLOCK_Q), F32),
                pltpu.VMEM((PAIR, keys), F32),
                pltpu.VMEM((PAIR, keys), F32),
            ],
        ),
        compiler_params=pltpu.CompilerParams(vmem_limit_bytes=VMEM_LIMIT),
        cost_estimate=cost(rows, keys, 10),
        name="attend_back",
    )(bounds, query, key, value, grad, query_tags, key_tags, lse, delta)


def head_stats(grad, out):
    rows, width = out.shape
    sums = jnp.sum((grad.astype(F32) * out.astype(F32)).reshape(rows, HEADS, HEAD_DIM), axis=2)
    pairs = sums.T.reshape(HEADS // 2, 2, rows)
    return jnp.pad(pairs, ((0, 0), (0, 6), (0, 0)))


def tag_lanes(kind, items):
    lane = jnp.arange(PAIR, dtype=jnp.int32)[None, :] % HEAD_DIM
    kind = jnp.where(kind < 0, items, kind)[:, None]
    key_tags = (lane == kind).astype(BF16)
    query_tags = jnp.where((lane != kind) & (lane <= items), PENALTY, 0.0).astype(BF16)
    return query_tags, key_tags


def layer_norm(values):
    centre = values - jnp.mean(values, axis=-1, keepdims=True)
    return centre * lax.rsqrt(jnp.mean(centre * centre, axis=-1, keepdims=True) + EPSILON)


def modulate(values, shift, scale):
    return layer_norm(values) * (1.0 + scale) + shift


def of_owner(owner, table):
    chosen = jnp.broadcast_to(table[0][None, :], (owner.shape[0], table.shape[1]))
    for item in range(1, table.shape[0]):
        chosen = jnp.where((owner == item)[:, None], table[item][None, :], chosen)
    return chosen


def per_item(owner, items, values):
    select = (jnp.arange(items, dtype=jnp.int32)[:, None] == owner[None, :]).astype(BF16)
    coarse = lax.reduce_precision(values, 8, 7)
    fine = lax.reduce_precision(values - coarse, 8, 7)
    return product(select, coarse.astype(BF16)) + product(select, fine.astype(BF16))


def shifted(x, axis, by):
    size = lax.axis_size(axis)
    return lax.ppermute(x, axis, [(i, (i + by) % size) for i in range(size)])


def neighbour(x, axis, by):
    size = lax.axis_size(axis)
    return lax.ppermute(x, axis, [(i, i + by) for i in range(size) if 0 <= i + by < size])


def to_slabs(matrix, groups, slab):
    rows, columns = matrix.shape[0] // groups, matrix.shape[1]
    split = matrix.reshape(groups, rows, columns)
    pieces = [split[:, i * slab : (i + 1) * slab] for i in range(rows // slab)]
    rest = rows % slab
    if rest:
        tail = split[:, rows - rest :].reshape(groups, rest, slab // rest, columns * rest // slab)
        pieces.append(tail.transpose(0, 2, 1, 3).reshape(groups, slab, columns * rest // slab))
    return jnp.concatenate(pieces, axis=2).reshape(groups * slab, -1)


def from_slab(packed, shape):
    slab, (rows, columns) = packed.shape[0], shape
    whole, rest = divmod(rows, slab)
    pieces = [packed[:, i * columns : (i + 1) * columns] for i in range(whole)]
    if rest:
        tail = packed[:, whole * columns :].reshape(slab // rest, rest, columns * rest // slab)
        pieces.append(tail.transpose(1, 0, 2).reshape(rest, columns))
    return jnp.concatenate(pieces, axis=0)


def scattered(grads, axis):
    return lax.psum_scatter(grads.astype(BF16), axis, scatter_dimension=0, tiled=True)


def body(
    frames, text_states, timestep, frame_lengths, text_lengths,
    cond_weight, cond_bias, joint_weight, self_output, query_weight, text_weight, cross_output,
    up_weight, up_bias, down_weight, down_bias, cotangent,
):
    rows, width = frames.shape
    parts, position = lax.axis_size("text"), lax.axis_index("text")
    groups, group = lax.axis_size("seq"), lax.axis_index("seq")
    items, tokens, text_width = text_states.shape
    mod_width = cond_weight.shape[1]

    small = jnp.concatenate([timestep.reshape(-1), cond_bias, up_bias, down_bias]).astype(F32)
    small_all = lax.all_gather(small[None, :], "seq", axis=0)[:, 0]
    joint_full = lax.all_gather(joint_weight, "seq", axis=0, tiled=True)
    text_full = lax.all_gather(text_weight, "seq", axis=0, tiled=True)
    outer_full = lax.all_gather(
        jnp.concatenate([self_output, query_weight, cross_output], axis=1), "seq", axis=0, tiled=True
    )
    up_full = lax.all_gather(up_weight, "seq", axis=0, tiled=True)
    down_full = lax.all_gather(down_weight, "seq", axis=0, tiled=True)
    before = neighbour(frames, "text", 1)
    after = neighbour(frames, "text", -1)
    flat_text = text_states.reshape(items * tokens, text_width)

    cut = timestep.size
    steps_all = small_all[:, :cut].reshape(groups * items, width)
    cond_bias_full = small_all[:, cut : cut + cond_bias.size].reshape(-1).astype(F32)
    cut += cond_bias.size
    up_bias_full = small_all[:, cut : cut + up_bias.size].reshape(-1).astype(F32)
    cut += up_bias.size
    down_bias_full = small_all[:, cut:].reshape(-1).astype(F32)

    silu_all = jax.nn.silu(steps_all.astype(F32)).astype(BF16)
    slab = cond_weight.shape[0]
    silu_mine = lax.dynamic_slice_in_dim(silu_all, group * slab, slab, axis=1)
    modulation = (
        lax.psum_scatter(product(silu_mine, cond_weight), "seq", scatter_dimension=0, tiled=True)
        + cond_bias_full
    )

    ends = jnp.cumsum(frame_lengths[0])
    starts = ends - frame_lengths[0]

    def item_of(places):
        inside = (places >= 0) & (places < rows * parts)
        found = jnp.sum((places[:, None] >= ends[None, :]).astype(jnp.int32), axis=1)
        return jnp.where(inside, found, -1)

    origin = (position - 1) * rows
    window_item = item_of(origin + jnp.arange(3 * rows, dtype=jnp.int32))
    own_item = window_item[rows : 2 * rows]
    token_index = jnp.arange(items * parts * tokens, dtype=jnp.int32)
    token_item = token_index // (parts * tokens)
    in_item = token_index % (parts * tokens)
    token_place = ((position - in_item // tokens) % parts) * tokens + in_item % tokens
    token_kind = jnp.where(token_place < text_lengths[token_item], token_item, -1)
    query_tags, _ = tag_lanes(own_item, items)
    _, window_tags = tag_lanes(window_item, items)
    _, token_tags = tag_lanes(token_kind, items)
    firsts = own_item[:: BLOCK_Q]
    lasts = own_item[BLOCK_Q - 1 :: BLOCK_Q]
    self_bounds = jnp.stack(
        [(starts[firsts] - origin) // BLOCK_K, (ends[lasts] - origin + BLOCK_K - 1) // BLOCK_K]
    )
    per_text = parts * tokens // BLOCK_K
    cross_bounds = jnp.stack([firsts * per_text, (lasts + 1) * per_text])

    late_text, before, after = lax.optimization_barrier((text_states, before, after))
    text_parts = [text_states] + [shifted(late_text, "text", k) for k in range(1, parts)]
    source = jnp.concatenate([before, frames, after], axis=0).astype(F32)
    own = slice(rows, 2 * rows)
    blocks = [modulation[:, i * width : (i + 1) * width] for i in range(6)]
    shift_one = of_owner(window_item, blocks[0])
    scale_one = of_owner(window_item, blocks[1])
    gate_one, shift_two, scale_two, gate_two = [of_owner(own_item, table) for table in blocks[2:]]
    normed_one = modulate(source, shift_one, scale_one).astype(BF16)
    factor = HEAD_DIM ** (-0.5)
    query = product(normed_one[own], joint_full[:, :width]).astype(BF16) * BF16(factor)
    keyvalue = product(normed_one, joint_full[:, width:]).astype(BF16)
    key, value = keyvalue[:, :width], keyvalue[:, width:]
    mixed, self_lse = attend(self_bounds, query, key, value, query_tags, window_tags)
    mixed, text_parts = lax.optimization_barrier((mixed, text_parts))
    output_full = outer_full[:, :width]
    query_full = outer_full[:, width : 2 * width]
    cross_full = outer_full[:, 2 * width :]
    self_branch = product(mixed, output_full)
    after_self = source[own] + gate_one * self_branch
    normed_two = layer_norm(after_self).astype(BF16)
    cross_query = product(normed_two, query_full).astype(BF16) * BF16(factor)
    text_all = jnp.concatenate(text_parts, axis=1).reshape(items * parts * tokens, text_width)
    text_kv = product(text_all, text_full).astype(BF16)
    text_key, text_value = text_kv[:, :width], text_kv[:, width:]
    cross_mixed, cross_lse = attend(
        cross_bounds, cross_query, text_key, text_value, query_tags, token_tags
    )
    after_cross = after_self + product(cross_mixed, cross_full)
    normed_three = modulate(after_cross, shift_two, scale_two).astype(BF16)
    hidden = product(normed_three, up_full) + up_bias_full
    activated = jax.nn.gelu(hidden, approximate=True).astype(BF16)
    mlp_branch = product(activated, down_full) + down_bias_full
    result = (after_cross + gate_two * mlp_branch).astype(BF16)

    upstream = cotangent.astype(F32)
    grad_gate_two = upstream * mlp_branch
    grad_branch = (gate_two * upstream).astype(BF16)
    grad_down = contract_first(activated, grad_branch).astype(BF16)
    grad_down_bias = jnp.sum(grad_branch.astype(F32), axis=0)
    grad_activated = contract_last(grad_branch, down_full)
    _, gelu_pull = jax.vjp(lambda entry: jax.nn.gelu(entry, approximate=True), hidden)
    grad_hidden = gelu_pull(grad_activated)[0].astype(BF16)
    grad_up = contract_first(normed_three, grad_hidden).astype(BF16)
    wide = jnp.concatenate([grad_up, to_slabs(grad_down, groups, slab)], axis=1)
    grad_up_bias = jnp.sum(grad_hidden.astype(F32), axis=0)
    grad_normed_three = contract_last(grad_hidden, up_full)
    _, third_pull = jax.vjp(modulate, after_cross, shift_two, scale_two)
    grad_after_cross, grad_shift_two, grad_scale_two = third_pull(grad_normed_three)
    grad_after_cross = grad_after_cross + upstream
    grad_cross_branch = grad_after_cross.astype(BF16)
    grad_cross_output = contract_first(cross_mixed, grad_cross_branch)
    grad_cross_mixed = contract_last(grad_cross_branch, cross_full).astype(BF16)
    grad_cross_mixed, wide = lax.optimization_barrier((grad_cross_mixed, wide))
    share_wide = scattered(wide, "seq")
    grad_cross_query, grad_text_key, grad_text_value = attend_back(
        cross_bounds, cross_query, text_key, text_value, grad_cross_mixed, query_tags, token_tags,
        cross_lse, head_stats(grad_cross_mixed, cross_mixed),
    )
    grad_text_kv = jnp.concatenate([grad_text_key, grad_text_value], axis=1)
    grad_text_weight = contract_first(text_all, grad_text_kv).astype(BF16)
    grad_text_all = contract_last(grad_text_kv, text_full).reshape(items, parts, tokens, text_width)
    grad_text = grad_text_all[:, 0]
    sent_text = [
        shifted(grad_text_all[:, k].astype(BF16), "text", -k) for k in range(1, parts)
    ]
    grad_query_weight = contract_first(normed_two, grad_cross_query)
    grad_normed_two = contract_last(grad_cross_query, query_full)
    _, norm_pull = jax.vjp(layer_norm, after_self)
    grad_after_self = grad_after_cross + norm_pull(grad_normed_two)[0]
    grad_gate_one = grad_after_self * self_branch
    grad_self_branch = (gate_one * grad_after_self).astype(BF16)
    grad_self_output = contract_first(mixed, grad_self_branch)
    mid = jnp.concatenate(
        [
            grad_self_output.astype(BF16), grad_query_weight.astype(BF16),
            grad_cross_output.astype(BF16), to_slabs(grad_text_weight, groups, slab),
        ],
        axis=1,
    )
    grad_mixed = contract_last(grad_self_branch, output_full).astype(BF16)
    grad_mixed, mid = lax.optimization_barrier((grad_mixed, mid))
    share_mid = scattered(mid, "seq")
    grad_query, grad_key, grad_value = attend_back(
        self_bounds, query, key, value, grad_mixed, query_tags, window_tags,
        self_lse, head_stats(grad_mixed, mixed),
    )
    grad_query, share_wide, sent_text = lax.optimization_barrier((grad_query, share_wide, sent_text))
    for sent in sent_text:
        grad_text = grad_text + sent.astype(F32)
    grad_keyvalue = jnp.concatenate([grad_key, grad_value], axis=1)
    share_joint = scattered(
        jnp.concatenate(
            [contract_first(normed_one[own], grad_query), contract_first(normed_one, grad_keyvalue)],
            axis=1,
        ),
        "seq",
    )
    grad_normed_one = contract_last(grad_keyvalue, joint_full[:, width:])
    grad_normed_own = contract_last(grad_query, joint_full[:, :width])
    grad_normed_one = jnp.concatenate(
        [grad_normed_one[:rows], grad_normed_one[own] + grad_normed_own, grad_normed_one[2 * rows :]]
    )
    _, first_pull = jax.vjp(modulate, source, shift_one, scale_one)
    grad_source, grad_shift_one, grad_scale_one = first_pull(grad_normed_one)
    summed_wide = lax.psum(share_wide, "text")
    share_mid, summed_wide, grad_source = lax.optimization_barrier(
        (share_mid, summed_wide, grad_source)
    )
    from_next = neighbour(grad_source[:rows].astype(BF16), "text", -1)
    from_previous = neighbour(grad_source[2 * rows :].astype(BF16), "text", 1)
    grad_frames = (
        grad_source[own] + grad_after_self + from_next.astype(F32) + from_previous.astype(F32)
    )
    late = per_item(window_item, items, jnp.concatenate([grad_shift_one, grad_scale_one], axis=1))
    early = per_item(
        own_item, items,
        jnp.concatenate([grad_gate_one, grad_shift_two, grad_scale_two, grad_gate_two], axis=1),
    )
    grad_modulation = jnp.concatenate([late, early], axis=1)
    sums = jnp.concatenate([grad_modulation.reshape(-1), grad_up_bias, grad_down_bias])
    summed_mid = lax.psum(share_mid, "text")
    share_joint, summed_mid = lax.optimization_barrier((share_joint, summed_mid))
    summed_joint = lax.psum(share_joint, "text").astype(F32)
    sums_all = lax.all_gather(lax.psum(sums, "text")[None, :], "seq", axis=0)[:, 0]
    cut = items * mod_width
    grad_mod_all = sums_all[:, :cut].reshape(groups * items, mod_width)
    grad_cond_weight = lax.dot_general(
        silu_mine.astype(F32), grad_mod_all, (((0,), (0,)), ((), ())), precision=lax.Precision.HIGHEST
    )
    grad_cond_bias = jnp.sum(
        lax.dynamic_slice_in_dim(grad_mod_all, group * cond_bias.size, cond_bias.size, axis=1), axis=0
    )
    bias_sums = jnp.sum(sums_all[:, cut:], axis=0)
    share_up_bias = lax.dynamic_slice_in_dim(
        bias_sums[: up_bias.size * groups], group * up_bias.size, up_bias.size
    )
    share_down_bias = lax.dynamic_slice_in_dim(
        bias_sums[up_bias.size * groups :], group * down_bias.size, down_bias.size
    )
    summed_wide, summed_mid = summed_wide.astype(F32), summed_mid.astype(F32)
    up_width = up_weight.shape[1]
    return (
        result, grad_frames, grad_text, grad_cond_weight, grad_cond_bias, summed_joint,
        summed_mid[:, :width], summed_mid[:, width : 2 * width],
        from_slab(summed_mid[:, 3 * width :], text_weight.shape), summed_mid[:, 2 * width : 3 * width],
        summed_wide[:, :up_width], share_up_bias,
        from_slab(summed_wide[:, up_width:], down_weight.shape), share_down_bias,
    )


def solution(mesh):
    both, seq, flat = P(("seq", "text"), None), P("seq", None), P("seq")
    texts = P("seq", "text", None)
    return jax.shard_map(
        body,
        mesh=mesh,
        in_specs=(
            both, texts, seq, seq, flat, seq, flat, seq, seq, seq, seq, seq, seq, flat, seq, flat, both,
        ),
        out_specs=(
            both, both, texts, seq, flat, seq, seq, seq, seq, seq, seq, flat, seq, flat,
        ),
        check_vma=False,
    )
```

```python
import functools

import jax
import jax.numpy as jnp
from jax import lax
from jax.experimental import pallas as pl
from jax.experimental.pallas import tpu as pltpu
from jax.sharding import PartitionSpec as P

HEADS = 12
HEAD_DIM = 64
PAIR = 2 * HEAD_DIM
EPSILON = 1e-06
BLOCK_Q = 256
BLOCK_K = 256
PENALTY = -1e30
VMEM_LIMIT = 60 * 1024 * 1024

BF16 = jnp.bfloat16
F32 = jnp.float32


def contract(left, right, dims):
    return lax.dot_general(left, right, (dims, ((), ())), preferred_element_type=F32)


def product(left, right):
    return contract(left, right, ((1,), (0,)))


def contract_first(left, right):
    return contract(left, right, ((0,), (0,)))


def contract_last(left, right):
    return contract(left, right, ((1,), (1,)))


def halves():
    lane = lax.broadcasted_iota(jnp.int32, (1, PAIR), 1)
    low = (lane < HEAD_DIM).astype(F32).astype(BF16)
    return low, (lane >= HEAD_DIM).astype(F32).astype(BF16)


def rows_of(block, size):
    return pl.ds(pl.multiple_of(block * size, size), size)


def span(bounds, i, key_blocks, wide):
    first, last = bounds[0, i], bounds[1, i]
    steps = (last - first + wide - 1) // wide
    return jnp.minimum(first, key_blocks - wide * steps), steps


def forward_kernel(wide, bounds, q_ref, k_ref, v_ref, qt_ref, kt_ref, o_ref, lse_ref, ka_ref, vt_ref):
    low, high = halves()
    key_blocks = k_ref.shape[0] // BLOCK_K
    ones = jnp.ones((16, BLOCK_K), F32).astype(BF16)

    @pl.loop(0, key_blocks)
    def _(b):
        rows = rows_of(b, BLOCK_K)
        keys, tags = k_ref[rows, :], kt_ref[rows, :]
        ka_ref[0, rows, :] = keys * low + tags * high
        ka_ref[1, rows, :] = keys * high + tags * low
        turned = v_ref[rows, :].astype(F32).T.astype(BF16)
        vt_ref[0, :HEAD_DIM, rows] = turned[:HEAD_DIM]
        vt_ref[1, :HEAD_DIM, rows] = turned[HEAD_DIM:]
        vt_ref[0, HEAD_DIM:, rows] = ones
        vt_ref[1, HEAD_DIM:, rows] = ones

    @pl.loop(0, q_ref.shape[0] // BLOCK_Q)
    def _(i):
        mine = rows_of(i, BLOCK_Q)
        queries, tags = q_ref[mine, :], qt_ref[mine, :]
        tagged = (queries * low + tags * high, queries * high + tags * low)
        first, steps = span(bounds, i, key_blocks, wide)

        def step(b, states):
            parts = [rows_of(first + wide * b + j, BLOCK_K) for j in range(wide)]
            scores = [[contract_last(ka_ref[h, rows, :], tagged[h]) for rows in parts] for h in range(2)]
            tops = []
            for h in range(2):
                top = states[h][0]
                for part in scores[h]:
                    top = jnp.maximum(top, jnp.max(part, axis=0, keepdims=True))
                tops.append(top)
            expos = [[jnp.exp(part - tops[h]).astype(BF16) for part in scores[h]] for h in range(2)]
            following = []
            for h in range(2):
                peak, acc = states[h]
                acc = acc * jnp.exp(peak - tops[h])
                for part, rows in zip(expos[h], parts):
                    acc = acc + product(vt_ref[h, :, rows], part)
                following.append((tops[h], acc))
            return tuple(following)

        start = (
            jnp.full((1, BLOCK_Q), 2 * PENALTY, F32),
            jnp.zeros((HEAD_DIM + 16, BLOCK_Q), F32),
        )
        ended = lax.fori_loop(0, steps, step, (start, start))
        totals = [acc[HEAD_DIM : HEAD_DIM + 1] for _, acc in ended]
        outs = [acc[:HEAD_DIM] / total for total, (_, acc) in zip(totals, ended)]
        o_ref[mine, :] = jnp.concatenate(outs, axis=0).T.astype(BF16)
        for h in range(2):
            lse_ref[0, h : h + 1, mine] = ended[h][0] + jnp.log(totals[h])


def backward_kernel(
    wide, bounds, q_ref, k_ref, v_ref, g_ref, o_ref, qt_ref, kt_ref, lse_ref,
    dq_ref, dk_ref, dv_ref, ka_ref, kt_s, dqt, dk_acc, dv_acc,
):
    low, high = halves()
    key_blocks = k_ref.shape[0] // BLOCK_K

    @pl.loop(0, key_blocks)
    def _(b):
        rows = rows_of(b, BLOCK_K)
        keys, tags = k_ref[rows, :], kt_ref[rows, :]
        ka_ref[0, rows, :] = keys * low + tags * high
        ka_ref[1, rows, :] = keys * high + tags * low
        kt_s[:, rows] = keys.astype(F32).T.astype(BF16)
        dk_acc[:, rows] = jnp.zeros((PAIR, BLOCK_K), F32)
        dv_acc[:, rows] = jnp.zeros((PAIR, BLOCK_K), F32)

    @pl.loop(0, q_ref.shape[0] // BLOCK_Q)
    def _(i):
        mine = rows_of(i, BLOCK_Q)
        queries, tags, grads = q_ref[mine, :], qt_ref[mine, :], g_ref[mine, :]
        tagged = (queries * low + tags * high, queries * high + tags * low)
        split = (grads * low, grads * high)
        q_turned = queries.astype(F32).T.astype(BF16)
        g_turned = grads.astype(F32).T
        pulls = g_turned * o_ref[mine, :].astype(F32).T
        deltas = [jnp.sum(pulls[:HEAD_DIM], axis=0, keepdims=True)]
        deltas.append(jnp.sum(pulls[HEAD_DIM:], axis=0, keepdims=True))
        g_turned = g_turned.astype(BF16)
        lses = [lse_ref[0, h : h + 1, mine] for h in range(2)]
        dqt[...] = jnp.zeros(dqt.shape, F32)
        first, steps = span(bounds, i, key_blocks, wide)

        @pl.loop(0, steps)
        def _(b):
            found = []
            for j in range(wide):
                rows = rows_of(first + wide * b + j, BLOCK_K)
                for h in range(2):
                    scores = contract_last(ka_ref[h, rows, :], tagged[h])
                    found.append((h, rows, scores, contract_last(v_ref[rows, :], split[h])))
            made = []
            for h, rows, scores, pull in found:
                expos = jnp.exp(scores - lses[h])
                slope = (expos * (pull - deltas[h])).astype(BF16)
                made.append((h, rows, expos.astype(BF16), slope))
            for h, rows, weight, slope in made:
                part = slice(h * HEAD_DIM, (h + 1) * HEAD_DIM)
                dk_acc[part, rows] += contract_last(q_turned[part], slope)
                dv_acc[part, rows] += contract_last(g_turned[part], weight)
                dqt[part, :] += product(kt_s[part, rows], slope)

        dq_ref[mine, :] = (dqt[...] * HEAD_DIM ** (-0.5)).T.astype(BF16)

    @pl.loop(0, key_blocks)
    def _(b):
        rows = rows_of(b, BLOCK_K)
        dk_ref[rows, :] = dk_acc[:, rows].T.astype(BF16)
        dv_ref[rows, :] = dv_acc[:, rows].T.astype(BF16)


def column(rows):
    return pl.BlockSpec((rows, PAIR), lambda j, *_: (0, j))


def shared(rows):
    return pl.BlockSpec((rows, PAIR), lambda j, *_: (0, 0))


def stat(rows):
    return pl.BlockSpec((1, 8, rows), lambda j, *_: (j, 0, 0))


def cost(rows, keys, matmuls):
    return pl.CostEstimate(
        flops=matmuls * rows * keys * HEADS * HEAD_DIM, bytes_accessed=8 * (rows + keys) * HEADS * HEAD_DIM,
        transcendentals=rows * keys * HEADS // 2,
    )


def attend(wide, bounds, query, key, value, query_tags, key_tags):
    rows, width = query.shape
    keys = key.shape[0]
    return pl.pallas_call(
        functools.partial(forward_kernel, wide),
        out_shape=(
            jax.ShapeDtypeStruct((rows, width), BF16),
            jax.ShapeDtypeStruct((width // PAIR, 8, rows), F32),
        ),
        grid_spec=pltpu.PrefetchScalarGridSpec(
            num_scalar_prefetch=1,
            grid=(width // PAIR,),
            in_specs=[column(rows), column(keys), column(keys), shared(rows), shared(keys)],
            out_specs=[column(rows), stat(rows)],
            scratch_shapes=[
                pltpu.VMEM((2, keys, PAIR), BF16),
                pltpu.VMEM((2, HEAD_DIM + 16, keys), BF16),
            ],
        ),
        compiler_params=pltpu.CompilerParams(vmem_limit_bytes=VMEM_LIMIT),
        cost_estimate=cost(rows, keys, 4),
        name="attend",
    )(bounds, query, key, value, query_tags, key_tags)


def attend_back(wide, bounds, query, key, value, grad, out, query_tags, key_tags, lse):
    rows, width = query.shape
    keys = key.shape[0]
    return pl.pallas_call(
        functools.partial(backward_kernel, wide),
        out_shape=(
            jax.ShapeDtypeStruct((rows, width), BF16),
            jax.ShapeDtypeStruct((keys, width), BF16),
            jax.ShapeDtypeStruct((keys, width), BF16),
        ),
        grid_spec=pltpu.PrefetchScalarGridSpec(
            num_scalar_prefetch=1,
            grid=(width // PAIR,),
            in_specs=[
                column(rows), column(keys), column(keys), column(rows), column(rows), shared(rows),
                shared(keys), stat(rows),
            ],
            out_specs=[column(rows), column(keys), column(keys)],
            scratch_shapes=[
                pltpu.VMEM((2, keys, PAIR), BF16),
                pltpu.VMEM((PAIR, keys), BF16),
                pltpu.VMEM((PAIR, BLOCK_Q), F32),
                pltpu.VMEM((PAIR, keys), F32),
                pltpu.VMEM((PAIR, keys), F32),
            ],
        ),
        compiler_params=pltpu.CompilerParams(vmem_limit_bytes=VMEM_LIMIT),
        cost_estimate=cost(rows, keys, 10),
        name="attend_back",
    )(bounds, query, key, value, grad, out, query_tags, key_tags, lse)


def tag_lanes(kind, items):
    lane = jnp.arange(PAIR, dtype=jnp.int32)[None, :] % HEAD_DIM
    kind = jnp.where(kind < 0, items, kind)[:, None]
    key_tags = (lane == kind).astype(BF16)
    query_tags = jnp.where((lane != kind) & (lane <= items), PENALTY, 0.0).astype(BF16)
    return query_tags, key_tags


def layer_norm(values):
    centre = values - jnp.mean(values, axis=-1, keepdims=True)
    return centre * lax.rsqrt(jnp.mean(centre * centre, axis=-1, keepdims=True) + EPSILON)


def modulate(values, shift, scale):
    return layer_norm(values) * (1.0 + scale) + shift


def of_owner(owner, table):
    chosen = jnp.broadcast_to(table[0][None, :], (owner.shape[0], table.shape[1]))
    for item in range(1, table.shape[0]):
        chosen = jnp.where((owner == item)[:, None], table[item][None, :], chosen)
    return chosen


def per_item(owner, items, values):
    select = (jnp.arange(items, dtype=jnp.int32)[:, None] == owner[None, :]).astype(BF16)
    coarse = lax.reduce_precision(values, 8, 7)
    fine = lax.reduce_precision(values - coarse, 8, 7)
    return product(select, coarse.astype(BF16)) + product(select, fine.astype(BF16))


def shifted(x, axis, by):
    size = lax.axis_size(axis)
    return lax.ppermute(x, axis, [(i, (i + by) % size) for i in range(size)])


def neighbour(x, axis, by):
    size = lax.axis_size(axis)
    return lax.ppermute(x, axis, [(i, i + by) for i in range(size) if 0 <= i + by < size])


def to_slabs(matrix, groups, slab):
    rows, columns = matrix.shape[0] // groups, matrix.shape[1]
    split = matrix.reshape(groups, rows, columns)
    pieces = [split[:, i * slab : (i + 1) * slab] for i in range(rows // slab)]
    rest = rows % slab
    if rest:
        tail = split[:, rows - rest :].reshape(groups, rest, slab // rest, columns * rest // slab)
        pieces.append(tail.transpose(0, 2, 1, 3).reshape(groups, slab, columns * rest // slab))
    return jnp.concatenate(pieces, axis=2).reshape(groups * slab, -1)


def from_slab(packed, shape):
    slab, (rows, columns) = packed.shape[0], shape
    whole, rest = divmod(rows, slab)
    pieces = [packed[:, i * columns : (i + 1) * columns] for i in range(whole)]
    if rest:
        tail = packed[:, whole * columns :].reshape(slab // rest, rest, columns * rest // slab)
        pieces.append(tail.transpose(1, 0, 2).reshape(rest, columns))
    return jnp.concatenate(pieces, axis=0)


def scattered(grads, axis):
    return lax.psum_scatter(grads.astype(BF16), axis, scatter_dimension=0, tiled=True)


def body(
    frames, text_states, timestep, frame_lengths, text_lengths,
    cond_weight, cond_bias, joint_weight, self_output, query_weight, text_weight, cross_output,
    up_weight, up_bias, down_weight, down_bias, cotangent,
):
    rows, width = frames.shape
    parts, position = lax.axis_size("text"), lax.axis_index("text")
    groups, group = lax.axis_size("seq"), lax.axis_index("seq")
    items, tokens, text_width = text_states.shape
    mod_width = cond_weight.shape[1]

    small = jnp.concatenate([timestep.reshape(-1), cond_bias, up_bias, down_bias]).astype(F32)
    small_all = lax.all_gather(small[None, :], "seq", axis=0)[:, 0]
    joint_full = lax.all_gather(joint_weight, "seq", axis=0, tiled=True)
    text_full = lax.all_gather(text_weight, "seq", axis=0, tiled=True)
    outer_full = lax.all_gather(
        jnp.concatenate([self_output, query_weight, cross_output], axis=1), "seq", axis=0, tiled=True
    )
    up_full = lax.all_gather(up_weight, "seq", axis=0, tiled=True)
    down_full = lax.all_gather(down_weight, "seq", axis=0, tiled=True)
    before = neighbour(frames, "text", 1)
    after = neighbour(frames, "text", -1)
    flat_text = text_states.reshape(items * tokens, text_width)

    cut = timestep.size
    steps_all = small_all[:, :cut].reshape(groups * items, width)
    cond_bias_full = small_all[:, cut : cut + cond_bias.size].reshape(-1).astype(F32)
    cut += cond_bias.size
    up_bias_full = small_all[:, cut : cut + up_bias.size].reshape(-1).astype(F32)
    cut += up_bias.size
    down_bias_full = small_all[:, cut:].reshape(-1).astype(F32)

    silu_all = jax.nn.silu(steps_all.astype(F32)).astype(BF16)
    slab = cond_weight.shape[0]
    silu_mine = lax.dynamic_slice_in_dim(silu_all, group * slab, slab, axis=1)
    modulation = (
        lax.psum_scatter(product(silu_mine, cond_weight), "seq", scatter_dimension=0, tiled=True)
        + cond_bias_full
    )

    ends = jnp.cumsum(frame_lengths[0])
    starts = ends - frame_lengths[0]

    def item_of(places):
        inside = (places >= 0) & (places < rows * parts)
        found = jnp.sum((places[:, None] >= ends[None, :]).astype(jnp.int32), axis=1)
        return jnp.where(inside, found, -1)

    origin = (position - 1) * rows
    window_item = item_of(origin + jnp.arange(3 * rows, dtype=jnp.int32))
    own_item = window_item[rows : 2 * rows]
    token_index = jnp.arange(items * parts * tokens, dtype=jnp.int32)
    token_item = token_index // (parts * tokens)
    in_item = token_index % (parts * tokens)
    token_place = ((position - in_item // tokens) % parts) * tokens + in_item % tokens
    token_kind = jnp.where(token_place < text_lengths[token_item], token_item, -1)
    query_tags, _ = tag_lanes(own_item, items)
    _, window_tags = tag_lanes(window_item, items)
    _, token_tags = tag_lanes(token_kind, items)
    firsts = own_item[:: BLOCK_Q]
    lasts = own_item[BLOCK_Q - 1 :: BLOCK_Q]
    self_bounds = jnp.stack(
        [(starts[firsts] - origin) // BLOCK_K, (ends[lasts] - origin + BLOCK_K - 1) // BLOCK_K]
    )
    per_text = parts * tokens // BLOCK_K
    cross_bounds = jnp.stack([firsts * per_text, (lasts + 1) * per_text])

    late_text, before, after = lax.optimization_barrier((text_states, before, after))
    text_parts = [text_states] + [shifted(late_text, "text", k) for k in range(1, parts)]
    source = jnp.concatenate([before, frames, after], axis=0).astype(F32)
    own = slice(rows, 2 * rows)
    blocks = [modulation[:, i * width : (i + 1) * width] for i in range(6)]
    shift_one = of_owner(window_item, blocks[0])
    scale_one = of_owner(window_item, blocks[1])
    gate_one, shift_two, scale_two, gate_two = [of_owner(own_item, table) for table in blocks[2:]]
    normed_one = modulate(source, shift_one, scale_one).astype(BF16)
    factor = HEAD_DIM ** (-0.5)
    query = product(normed_one[own], joint_full[:, :width]).astype(BF16) * BF16(factor)
    keyvalue = product(normed_one, joint_full[:, width:]).astype(BF16)
    key, value = keyvalue[:, :width], keyvalue[:, width:]
    mixed, self_lse = attend(2, self_bounds, query, key, value, query_tags, window_tags)
    mixed, text_parts = lax.optimization_barrier((mixed, text_parts))
    output_full = outer_full[:, :width]
    query_full = outer_full[:, width : 2 * width]
    cross_full = outer_full[:, 2 * width :]
    self_branch = product(mixed, output_full)
    after_self = source[own] + gate_one * self_branch
    normed_two = layer_norm(after_self).astype(BF16)
    cross_query = product(normed_two, query_full).astype(BF16) * BF16(factor)
    text_all = jnp.concatenate(text_parts, axis=1).reshape(items * parts * tokens, text_width)
    text_kv = product(text_all, text_full).astype(BF16)
    text_key, text_value = text_kv[:, :width], text_kv[:, width:]
    cross_mixed, cross_lse = attend(
        1, cross_bounds, cross_query, text_key, text_value, query_tags, token_tags
    )
    after_cross = after_self + product(cross_mixed, cross_full)
    normed_three = modulate(after_cross, shift_two, scale_two).astype(BF16)
    hidden = product(normed_three, up_full) + up_bias_full
    activated = jax.nn.gelu(hidden, approximate=True).astype(BF16)
    mlp_branch = product(activated, down_full) + down_bias_full
    result = (after_cross + gate_two * mlp_branch).astype(BF16)

    upstream = cotangent.astype(F32)
    grad_gate_two = upstream * mlp_branch
    grad_branch = (gate_two * upstream).astype(BF16)
    grad_down = contract_first(activated, grad_branch).astype(BF16)
    grad_down_bias = jnp.sum(grad_branch.astype(F32), axis=0)
    grad_activated = contract_last(grad_branch, down_full)
    _, gelu_pull = jax.vjp(lambda entry: jax.nn.gelu(entry, approximate=True), hidden)
    grad_hidden = gelu_pull(grad_activated)[0].astype(BF16)
    grad_up = contract_first(normed_three, grad_hidden).astype(BF16)
    wide = jnp.concatenate([grad_up, to_slabs(grad_down, groups, slab)], axis=1)
    grad_up_bias = jnp.sum(grad_hidden.astype(F32), axis=0)
    grad_normed_three = contract_last(grad_hidden, up_full)
    _, third_pull = jax.vjp(modulate, after_cross, shift_two, scale_two)
    grad_after_cross, grad_shift_two, grad_scale_two = third_pull(grad_normed_three)
    grad_after_cross = grad_after_cross + upstream
    grad_cross_branch = grad_after_cross.astype(BF16)
    grad_cross_output = contract_first(cross_mixed, grad_cross_branch)
    grad_cross_mixed = contract_last(grad_cross_branch, cross_full).astype(BF16)
    grad_cross_mixed, wide = lax.optimization_barrier((grad_cross_mixed, wide))
    share_wide = scattered(wide, "seq")
    grad_cross_query, grad_text_key, grad_text_value = attend_back(
        1, cross_bounds, cross_query, text_key, text_value, grad_cross_mixed, cross_mixed,
        query_tags, token_tags, cross_lse,
    )
    grad_text_kv = jnp.concatenate([grad_text_key, grad_text_value], axis=1)
    grad_text_weight = contract_first(text_all, grad_text_kv).astype(BF16)
    grad_text_all = contract_last(grad_text_kv, text_full).reshape(items, parts, tokens, text_width)
    grad_text = grad_text_all[:, 0]
    sent_text = [
        shifted(grad_text_all[:, k].astype(BF16), "text", -k) for k in range(1, parts)
    ]
    grad_query_weight = contract_first(normed_two, grad_cross_query)
    grad_normed_two = contract_last(grad_cross_query, query_full)
    _, norm_pull = jax.vjp(layer_norm, after_self)
    grad_after_self = grad_after_cross + norm_pull(grad_normed_two)[0]
    grad_gate_one = grad_after_self * self_branch
    grad_self_branch = (gate_one * grad_after_self).astype(BF16)
    grad_self_output = contract_first(mixed, grad_self_branch)
    mid = jnp.concatenate(
        [
            grad_self_output.astype(BF16), grad_query_weight.astype(BF16),
            grad_cross_output.astype(BF16), to_slabs(grad_text_weight, groups, slab),
        ],
        axis=1,
    )
    grad_mixed = contract_last(grad_self_branch, output_full).astype(BF16)
    early = per_item(
        own_item, items,
        jnp.concatenate([grad_gate_one, grad_shift_two, grad_scale_two, grad_gate_two], axis=1),
    )
    early = jnp.concatenate([early.reshape(-1), grad_up_bias, grad_down_bias]).astype(BF16)
    grad_mixed, mid, share_wide, early = lax.optimization_barrier(
        (grad_mixed, mid, share_wide, early)
    )
    share_mid = scattered(mid, "seq")
    summed_wide, early = lax.psum((share_wide, early[None, :]), "text")
    grad_query, grad_key, grad_value = attend_back(
        2, self_bounds, query, key, value, grad_mixed, mixed, query_tags, window_tags, self_lse,
    )
    grad_query, sent_text, share_mid = lax.optimization_barrier((grad_query, sent_text, share_mid))
    for sent in sent_text:
        grad_text = grad_text + sent.astype(F32)
    grad_keyvalue = jnp.concatenate([grad_key, grad_value], axis=1)
    joint = jnp.concatenate(
        [
            contract_first(normed_one[own], grad_query).astype(BF16),
            contract_first(normed_one, grad_keyvalue).astype(BF16),
        ],
        axis=1,
    )
    grad_query, grad_keyvalue, joint = lax.optimization_barrier((grad_query, grad_keyvalue, joint))
    share_joint = scattered(joint, "seq")
    grad_normed_one = contract_last(grad_keyvalue, joint_full[:, width:])
    grad_normed_own = contract_last(grad_query, joint_full[:, :width])
    grad_normed_one = jnp.concatenate(
        [grad_normed_one[:rows], grad_normed_one[own] + grad_normed_own, grad_normed_one[2 * rows :]]
    )
    _, first_pull = jax.vjp(modulate, source, shift_one, scale_one)
    grad_source, grad_shift_one, grad_scale_one = first_pull(grad_normed_one)
    from_next = neighbour(grad_source[:rows].astype(BF16), "text", -1)
    from_previous = neighbour(grad_source[2 * rows :].astype(BF16), "text", 1)
    grad_frames = (
        grad_source[own] + grad_after_self + from_next.astype(F32) + from_previous.astype(F32)
    )
    late = per_item(window_item, items, jnp.concatenate([grad_shift_one, grad_scale_one], axis=1))
    late = late.reshape(1, -1).astype(BF16)
    share_mid, share_joint, late, summed_wide, early = lax.optimization_barrier(
        (share_mid, share_joint, late, summed_wide, early)
    )
    summed_mid, summed_joint, late = lax.psum((share_mid, share_joint, late), "text")
    summed_joint = summed_joint.astype(F32)
    sums_all = lax.all_gather(jnp.concatenate([late, early], axis=1).astype(F32), "seq", axis=0)[:, 0]
    cut = items * mod_width
    half = late.size
    grad_mod_all = jnp.concatenate(
        [
            sums_all[:, :half].reshape(groups * items, -1),
            sums_all[:, half:cut].reshape(groups * items, -1),
        ],
        axis=1,
    )
    grad_cond_weight = lax.dot_general(
        silu_mine.astype(F32), grad_mod_all, (((0,), (0,)), ((), ())), precision=lax.Precision.HIGHEST
    )
    grad_cond_bias = jnp.sum(
        lax.dynamic_slice_in_dim(grad_mod_all, group * cond_bias.size, cond_bias.size, axis=1), axis=0
    )
    bias_sums = jnp.sum(sums_all[:, cut:], axis=0)
    share_up_bias = lax.dynamic_slice_in_dim(
        bias_sums[: up_bias.size * groups], group * up_bias.size, up_bias.size
    )
    share_down_bias = lax.dynamic_slice_in_dim(
        bias_sums[up_bias.size * groups :], group * down_bias.size, down_bias.size
    )
    summed_wide, summed_mid = summed_wide.astype(F32), summed_mid.astype(F32)
    up_width = up_weight.shape[1]
    return (
        result, grad_frames, grad_text, grad_cond_weight, grad_cond_bias, summed_joint,
        summed_mid[:, :width], summed_mid[:, width : 2 * width],
        from_slab(summed_mid[:, 3 * width :], text_weight.shape), summed_mid[:, 2 * width : 3 * width],
        summed_wide[:, :up_width], share_up_bias,
        from_slab(summed_wide[:, up_width:], down_weight.shape), share_down_bias,
    )


def solution(mesh):
    both, seq, flat = P(("seq", "text"), None), P("seq", None), P("seq")
    texts = P("seq", "text", None)
    return jax.shard_map(
        body,
        mesh=mesh,
        in_specs=(
            both, texts, seq, seq, flat, seq, flat, seq, seq, seq, seq, seq, seq, flat, seq, flat, both,
        ),
        out_specs=(
            both, both, texts, seq, flat, seq, seq, seq, seq, seq, seq, flat, seq, flat,
        ),
        check_vma=False,
    )
```

```python
import functools

import jax
import jax.numpy as jnp
from jax import lax
from jax.experimental import pallas as pl
from jax.experimental.pallas import tpu as pltpu
from jax.sharding import PartitionSpec as P

HEADS = 12
HEAD_DIM = 64
PAIR = 2 * HEAD_DIM
EPSILON = 1e-06
BLOCK_Q = 256
BLOCK_K = 256
PENALTY = -1e30
VMEM_LIMIT = 60 * 1024 * 1024

BF16 = jnp.bfloat16
F32 = jnp.float32


def contract(left, right, dims):
    return lax.dot_general(left, right, (dims, ((), ())), preferred_element_type=F32)


def product(left, right):
    return contract(left, right, ((1,), (0,)))


def contract_first(left, right):
    return contract(left, right, ((0,), (0,)))


def contract_last(left, right):
    return contract(left, right, ((1,), (1,)))


def halves():
    lane = lax.broadcasted_iota(jnp.int32, (1, PAIR), 1)
    low = (lane < HEAD_DIM).astype(F32).astype(BF16)
    return low, (lane >= HEAD_DIM).astype(F32).astype(BF16)


def rows_of(block, size):
    return pl.ds(pl.multiple_of(block * size, size), size)


def span(bounds, i, key_blocks, wide):
    first, last = bounds[0, i], bounds[1, i]
    steps = (last - first + wide - 1) // wide
    return jnp.minimum(first, key_blocks - wide * steps), steps


def forward_kernel(wide, bounds, q_ref, kv_ref, qt_ref, kt_ref, o_ref, lse_ref, ka_ref, vt_ref):
    low, high = halves()
    key_blocks = kv_ref.shape[0] // BLOCK_K
    ones = jnp.ones((16, BLOCK_K), F32).astype(BF16)

    @pl.loop(0, key_blocks)
    def _(b):
        rows = rows_of(b, BLOCK_K)
        keys, tags = kv_ref[rows, :PAIR], kt_ref[rows, :]
        ka_ref[0, rows, :] = keys * low + tags * high
        ka_ref[1, rows, :] = keys * high + tags * low
        turned = kv_ref[rows, PAIR:].astype(F32).T.astype(BF16)
        vt_ref[0, :HEAD_DIM, rows] = turned[:HEAD_DIM]
        vt_ref[1, :HEAD_DIM, rows] = turned[HEAD_DIM:]
        vt_ref[0, HEAD_DIM:, rows] = ones
        vt_ref[1, HEAD_DIM:, rows] = ones

    @pl.loop(0, q_ref.shape[0] // BLOCK_Q)
    def _(i):
        mine = rows_of(i, BLOCK_Q)
        queries, tags = q_ref[mine, :], qt_ref[mine, :]
        tagged = (queries * low + tags * high, queries * high + tags * low)
        first, steps = span(bounds, i, key_blocks, wide)

        def step(b, states):
            parts = [rows_of(first + wide * b + j, BLOCK_K) for j in range(wide)]
            scores = [[contract_last(ka_ref[h, rows, :], tagged[h]) for rows in parts] for h in range(2)]
            tops = []
            for h in range(2):
                top = states[h][0]
                for part in scores[h]:
                    top = jnp.maximum(top, jnp.max(part, axis=0, keepdims=True))
                tops.append(top)
            expos = [[jnp.exp(part - tops[h]).astype(BF16) for part in scores[h]] for h in range(2)]
            following = []
            for h in range(2):
                peak, acc = states[h]
                acc = acc * jnp.exp(peak - tops[h])
                for part, rows in zip(expos[h], parts):
                    acc = acc + product(vt_ref[h, :, rows], part)
                following.append((tops[h], acc))
            return tuple(following)

        start = (
            jnp.full((1, BLOCK_Q), 2 * PENALTY, F32),
            jnp.zeros((HEAD_DIM + 16, BLOCK_Q), F32),
        )
        ended = lax.fori_loop(0, steps, step, (start, start))
        totals = [acc[HEAD_DIM : HEAD_DIM + 1] for _, acc in ended]
        outs = [acc[:HEAD_DIM] / total for total, (_, acc) in zip(totals, ended)]
        o_ref[mine, :] = jnp.concatenate(outs, axis=0).T.astype(BF16)
        for h in range(2):
            lse_ref[0, h : h + 1, mine] = ended[h][0] + jnp.log(totals[h])


def backward_kernel(
    wide, bounds, q_ref, kv_ref, g_ref, o_ref, qt_ref, kt_ref, lse_ref,
    dq_ref, dkv_ref, ka_ref, kt_s, dqt, dk_acc, dv_acc,
):
    low, high = halves()
    key_blocks = kv_ref.shape[0] // BLOCK_K

    @pl.loop(0, key_blocks)
    def _(b):
        rows = rows_of(b, BLOCK_K)
        keys, tags = kv_ref[rows, :PAIR], kt_ref[rows, :]
        ka_ref[0, rows, :] = keys * low + tags * high
        ka_ref[1, rows, :] = keys * high + tags * low
        kt_s[:, rows] = keys.astype(F32).T.astype(BF16)
        dk_acc[:, rows] = jnp.zeros((PAIR, BLOCK_K), F32)
        dv_acc[:, rows] = jnp.zeros((PAIR, BLOCK_K), F32)

    @pl.loop(0, q_ref.shape[0] // BLOCK_Q)
    def _(i):
        mine = rows_of(i, BLOCK_Q)
        queries, tags, grads = q_ref[mine, :], qt_ref[mine, :], g_ref[mine, :]
        tagged = (queries * low + tags * high, queries * high + tags * low)
        split = (grads * low, grads * high)
        q_turned = queries.astype(F32).T.astype(BF16)
        g_turned = grads.astype(F32).T
        pulls = g_turned * o_ref[mine, :].astype(F32).T
        deltas = [jnp.sum(pulls[:HEAD_DIM], axis=0, keepdims=True)]
        deltas.append(jnp.sum(pulls[HEAD_DIM:], axis=0, keepdims=True))
        g_turned = g_turned.astype(BF16)
        lses = [lse_ref[0, h : h + 1, mine] for h in range(2)]
        dqt[...] = jnp.zeros(dqt.shape, F32)
        first, steps = span(bounds, i, key_blocks, wide)

        @pl.loop(0, steps)
        def _(b):
            found = []
            for j in range(wide):
                rows = rows_of(first + wide * b + j, BLOCK_K)
                for h in range(2):
                    scores = contract_last(ka_ref[h, rows, :], tagged[h])
                    found.append((h, rows, scores, contract_last(kv_ref[rows, PAIR:], split[h])))
            made = []
            for h, rows, scores, pull in found:
                expos = jnp.exp(scores - lses[h])
                slope = (expos * (pull - deltas[h])).astype(BF16)
                made.append((h, rows, expos.astype(BF16), slope))
            for h, rows, weight, slope in made:
                part = slice(h * HEAD_DIM, (h + 1) * HEAD_DIM)
                dk_acc[part, rows] += contract_last(q_turned[part], slope)
                dv_acc[part, rows] += contract_last(g_turned[part], weight)
                dqt[part, :] += product(kt_s[part, rows], slope)

        dq_ref[mine, :] = (dqt[...] * HEAD_DIM ** (-0.5)).T.astype(BF16)

    @pl.loop(0, key_blocks)
    def _(b):
        rows = rows_of(b, BLOCK_K)
        dkv_ref[rows, :PAIR] = dk_acc[:, rows].T.astype(BF16)
        dkv_ref[rows, PAIR:] = dv_acc[:, rows].T.astype(BF16)


def column(rows):
    return pl.BlockSpec((rows, PAIR), lambda j, *_: (0, j))


def double(rows):
    return pl.BlockSpec((rows, 2 * PAIR), lambda j, *_: (0, j))


def shared(rows):
    return pl.BlockSpec((rows, PAIR), lambda j, *_: (0, 0))


def stat(rows):
    return pl.BlockSpec((1, 8, rows), lambda j, *_: (j, 0, 0))


def cost(rows, keys, matmuls):
    return pl.CostEstimate(
        flops=matmuls * rows * keys * HEADS * HEAD_DIM, bytes_accessed=8 * (rows + keys) * HEADS * HEAD_DIM,
        transcendentals=rows * keys * HEADS // 2,
    )


def attend(wide, bounds, query, keyvalue, query_tags, key_tags):
    rows, width = query.shape
    keys = keyvalue.shape[0]
    return pl.pallas_call(
        functools.partial(forward_kernel, wide),
        out_shape=(
            jax.ShapeDtypeStruct((rows, width), BF16),
            jax.ShapeDtypeStruct((width // PAIR, 8, rows), F32),
        ),
        grid_spec=pltpu.PrefetchScalarGridSpec(
            num_scalar_prefetch=1,
            grid=(width // PAIR,),
            in_specs=[column(rows), double(keys), shared(rows), shared(keys)],
            out_specs=[column(rows), stat(rows)],
            scratch_shapes=[
                pltpu.VMEM((2, keys, PAIR), BF16),
                pltpu.VMEM((2, HEAD_DIM + 16, keys), BF16),
            ],
        ),
        compiler_params=pltpu.CompilerParams(vmem_limit_bytes=VMEM_LIMIT),
        cost_estimate=cost(rows, keys, 4),
        name="attend",
    )(bounds, query, keyvalue, query_tags, key_tags)


def attend_back(wide, bounds, query, keyvalue, grad, out, query_tags, key_tags, lse):
    rows, width = query.shape
    keys = keyvalue.shape[0]
    return pl.pallas_call(
        functools.partial(backward_kernel, wide),
        out_shape=(
            jax.ShapeDtypeStruct((rows, width), BF16),
            jax.ShapeDtypeStruct((keys, 2 * width), BF16),
        ),
        grid_spec=pltpu.PrefetchScalarGridSpec(
            num_scalar_prefetch=1,
            grid=(width // PAIR,),
            in_specs=[
                column(rows), double(keys), column(rows), column(rows), shared(rows), shared(keys),
                stat(rows),
            ],
            out_specs=[column(rows), double(keys)],
            scratch_shapes=[
                pltpu.VMEM((2, keys, PAIR), BF16),
                pltpu.VMEM((PAIR, keys), BF16),
                pltpu.VMEM((PAIR, BLOCK_Q), F32),
                pltpu.VMEM((PAIR, keys), F32),
                pltpu.VMEM((PAIR, keys), F32),
            ],
        ),
        compiler_params=pltpu.CompilerParams(vmem_limit_bytes=VMEM_LIMIT),
        cost_estimate=cost(rows, keys, 10),
        name="attend_back",
    )(bounds, query, keyvalue, grad, out, query_tags, key_tags, lse)


TILE = 256
COPIES = 3
SLOTS = 8


def normed(values):
    centre = values - jnp.mean(values, axis=-1, keepdims=True)
    scale = lax.rsqrt(jnp.mean(centre * centre, axis=-1, keepdims=True) + EPSILON)
    return centre * scale, scale


def take(tile, own, before_ref, frames_ref, after_ref, x_ref):
    inside = (tile >= own[0]) & (tile < own[1])
    for chosen, ref in ((tile < own[0], before_ref), (inside, frames_ref), (tile >= own[1], after_ref)):

        @pl.when(chosen)
        def _(ref=ref):
            x_ref[...] = ref[...].astype(F32)


def window_tiles(width, first, last):
    def at(start, count):
        return tiles(width, lambda t: jnp.clip(t - start, 0, count - 1))

    return [at(0, first), at(first, last - first), at(last, first)]


def enter_kernel(own, before_ref, frames_ref, after_ref, sel_ref, shift_ref, scale_ref, w_ref, h_ref, q_ref, kv_ref, x_ref):
    tile = pl.program_id(0)
    width = x_ref.shape[1]
    take(tile, own, before_ref, frames_ref, after_ref, x_ref)
    norm, _ = normed(x_ref[...])
    select = sel_ref[...]
    values = norm * product(select, scale_ref[...]) + product(select, shift_ref[...])
    values = values.astype(BF16)
    h_ref[...] = values
    kv_ref[...] = product(values, w_ref[:, width:]).astype(BF16)

    @pl.when((tile >= own[0]) & (tile < own[1]))
    def _():
        q_ref[...] = (product(values, w_ref[:, :width]) * HEAD_DIM ** (-0.5)).astype(BF16)


def leave_kernel(
    own, dq_ref, dkv_ref, w_ref, before_ref, frames_ref, after_ref, sel_ref, scale_ref, add_ref, branch_ref,
    own_ref, halo_ref, sums_ref, gh_ref, x_ref,
):
    tile = pl.program_id(0)
    width = x_ref.shape[1]
    mine = (tile >= own[0]) & (tile < own[1])

    @pl.when(tile == 0)
    def _():
        sums_ref[...] = jnp.zeros(sums_ref.shape, F32)

    gh_ref[...] = contract_last(dkv_ref[...], w_ref[:, width:])

    @pl.when(mine)
    def _():
        gh_ref[...] += contract_last(dq_ref[...], w_ref[:, :width])

    take(tile, own, before_ref, frames_ref, after_ref, x_ref)
    grad = gh_ref[...]
    norm, scale = normed(x_ref[...])
    select = sel_ref[...]
    add_sums(sums_ref, select, grad, grad * norm)
    moved = grad * product(select, scale_ref[...])
    moved = norm_back(moved, norm, scale)

    @pl.when(mine)
    def _():
        own_ref[...] = moved + add_ref[...]
        add_sums(sums_ref, select, add_ref[...] * branch_ref[...], at=2)

    @pl.when(jnp.logical_not(mine))
    def _():
        halo_ref[...] = moved.astype(BF16)


def norm_back(grad, norm, scale):
    inner = jnp.mean(grad * norm, axis=-1, keepdims=True)
    return scale * (grad - jnp.mean(grad, axis=-1, keepdims=True) - norm * inner)


def add_sums(sums_ref, select, *terms, at=0):
    for slot, values in enumerate(terms, at):
        coarse = values.astype(BF16)
        fine = (values - coarse.astype(F32)).astype(BF16)
        total = contract_first(select, coarse) + contract_first(select, fine)
        sums_ref[slot * SLOTS : (slot + 1) * SLOTS, :] += total[:SLOTS]


def third_kernel(g_ref, w_ref, x_ref, sel_ref, scale_ref, add_ref, branch_ref, out_ref, sums_ref):
    @pl.when(pl.program_id(0) == 0)
    def _():
        sums_ref[...] = jnp.zeros(sums_ref.shape, F32)

    grad = contract_last(g_ref[...], w_ref[...])
    norm, scale = normed(x_ref[...])
    select = sel_ref[...]
    addend = add_ref[...].astype(F32)
    add_sums(sums_ref, select, grad, grad * norm, addend * branch_ref[...])
    moved = grad * product(select, scale_ref[...])
    out_ref[...] = norm_back(moved, norm, scale) + addend


def tiles(width, at=lambda t: t):
    return pl.BlockSpec((TILE, width), lambda t: (at(t), 0))


def whole(array):
    return pl.BlockSpec(array.shape, lambda t: (0, 0), pipeline_mode=pl.Buffered(1))


def enter(window, select, shift, scale, weight):
    rows, width = window[1].shape
    count = 3 * rows
    first, last = rows // TILE, 2 * rows // TILE
    return pl.pallas_call(
        functools.partial(enter_kernel, (first, last)),
        grid=(count // TILE,),
        out_shape=(
            jax.ShapeDtypeStruct((count, width), BF16),
            jax.ShapeDtypeStruct((rows, width), BF16),
            jax.ShapeDtypeStruct((count, 2 * width), BF16),
        ),
        in_specs=[
            *window_tiles(width, first, last), tiles(PAIR), whole(shift), whole(scale), whole(weight),
        ],
        out_specs=[
            tiles(width), tiles(width, lambda t: jnp.clip(t - first, 0, last - first - 1)), tiles(2 * width),
        ],
        scratch_shapes=[pltpu.VMEM((TILE, width), F32)],
        compiler_params=pltpu.CompilerParams(vmem_limit_bytes=VMEM_LIMIT),
        cost_estimate=pl.CostEstimate(
            flops=6 * count * width * width, bytes_accessed=8 * count * width, transcendentals=0
        ),
        name="enter",
    )(*window, select, shift, scale, weight)


def leave(grad_query, grad_keyvalue, weight, window, select, scale, addend, branch):
    rows, width = grad_query.shape
    count = 3 * rows
    first, last = rows // TILE, 2 * rows // TILE

    def own(t):
        return jnp.clip(t - first, 0, last - first - 1)

    def halo(t):
        return jnp.where(t < first, t, jnp.maximum(t - (last - first), first - 1))

    return pl.pallas_call(
        functools.partial(leave_kernel, (first, last)),
        grid=(count // TILE,),
        out_shape=(
            jax.ShapeDtypeStruct((rows, width), F32),
            jax.ShapeDtypeStruct((count - rows, width), BF16),
            jax.ShapeDtypeStruct((3 * SLOTS, width), F32),
        ),
        in_specs=[
            tiles(width, own), tiles(2 * width), whole(weight), *window_tiles(width, first, last),
            tiles(PAIR), whole(scale), tiles(width, own), tiles(width, own),
        ],
        out_specs=[
            tiles(width, own), tiles(width, halo), pl.BlockSpec((3 * SLOTS, width), lambda t: (0, 0)),
        ],
        scratch_shapes=[pltpu.VMEM((TILE, width), F32), pltpu.VMEM((TILE, width), F32)],
        compiler_params=pltpu.CompilerParams(vmem_limit_bytes=VMEM_LIMIT),
        cost_estimate=pl.CostEstimate(
            flops=6 * count * width * width, bytes_accessed=8 * count * width, transcendentals=0
        ),
        name="leave",
    )(grad_query, grad_keyvalue, weight, *window, select, scale, addend, branch)


def third(grad, weight, values, select, scale, addend, branch):
    rows, width = values.shape
    return pl.pallas_call(
        third_kernel,
        grid=(rows // TILE,),
        out_shape=(
            jax.ShapeDtypeStruct((rows, width), F32),
            jax.ShapeDtypeStruct((3 * SLOTS, width), F32),
        ),
        in_specs=[
            tiles(grad.shape[1]), whole(weight), tiles(width), tiles(PAIR), whole(scale), tiles(width),
            tiles(width),
        ],
        out_specs=[tiles(width), pl.BlockSpec((3 * SLOTS, width), lambda t: (0, 0))],
        compiler_params=pltpu.CompilerParams(vmem_limit_bytes=VMEM_LIMIT),
        cost_estimate=pl.CostEstimate(
            flops=2 * rows * width * grad.shape[1], bytes_accessed=16 * rows * width, transcendentals=0
        ),
        name="third",
    )(grad, weight, values, select, scale, addend, branch)


def outer_kernel(*refs):
    lefts, rights, slab_ref, out_ref, acc_ref = refs[:3], refs[3:6], refs[6], refs[7], refs[8]
    width = lefts[0].shape[1]

    @pl.when(pl.program_id(0) == 0)
    def _():
        acc_ref[...] = jnp.zeros(acc_ref.shape, F32)

    for i, (left, right) in enumerate(zip(lefts, rights)):
        acc_ref[:, i * width : (i + 1) * width] += contract_first(left[...], right[...])

    @pl.when(pl.program_id(0) == pl.num_programs(0) - 1)
    def _():
        out_ref[:, : 3 * width] = acc_ref[...].astype(BF16)
        out_ref[:, 3 * width :] = slab_ref[...]


def outer_grads(lefts, rights, slab):
    rows, width = lefts[0].shape
    shape = (width, 3 * width + slab.shape[1])
    return pl.pallas_call(
        outer_kernel,
        grid=(rows // TILE,),
        out_shape=jax.ShapeDtypeStruct(shape, BF16),
        in_specs=[tiles(width)] * 6 + [whole(slab)],
        out_specs=pl.BlockSpec(shape, lambda t: (0, 0)),
        scratch_shapes=[pltpu.VMEM((width, 3 * width), F32)],
        compiler_params=pltpu.CompilerParams(vmem_limit_bytes=VMEM_LIMIT),
        cost_estimate=pl.CostEstimate(
            flops=6 * rows * width * width, bytes_accessed=12 * rows * width + 4 * shape[0] * shape[1],
            transcendentals=0,
        ),
        name="outer_grads",
    )(*lefts, *rights, slab)


def selector(owner):
    lane = jnp.arange(PAIR, dtype=jnp.int32)[None, :]
    return ((lane < COPIES * SLOTS) & (lane % SLOTS == owner[:, None])).astype(BF16)


def exact_table(table):
    left = jnp.pad(table, ((0, SLOTS - table.shape[0]), (0, 0)))
    pieces = []
    for _ in range(COPIES):
        pieces.append(lax.reduce_precision(left, 8, 7))
        left = left - pieces[-1]
    return jnp.pad(jnp.concatenate(pieces, axis=0), ((0, PAIR - COPIES * SLOTS), (0, 0))).astype(BF16)


def tag_lanes(kind, items):
    lane = jnp.arange(PAIR, dtype=jnp.int32)[None, :] % HEAD_DIM
    kind = jnp.where(kind < 0, items, kind)[:, None]
    key_tags = (lane == kind).astype(BF16)
    query_tags = jnp.where((lane != kind) & (lane <= items), PENALTY, 0.0).astype(BF16)
    return query_tags, key_tags


def layer_norm(values):
    centre = values - jnp.mean(values, axis=-1, keepdims=True)
    return centre * lax.rsqrt(jnp.mean(centre * centre, axis=-1, keepdims=True) + EPSILON)


def modulate(values, shift, scale):
    return layer_norm(values) * (1.0 + scale) + shift


def of_owner(owner, table):
    chosen = jnp.broadcast_to(table[0][None, :], (owner.shape[0], table.shape[1]))
    for item in range(1, table.shape[0]):
        chosen = jnp.where((owner == item)[:, None], table[item][None, :], chosen)
    return chosen


def shifted(x, axis, by):
    size = lax.axis_size(axis)
    return lax.ppermute(x, axis, [(i, (i + by) % size) for i in range(size)])


def neighbour(x, axis, by):
    size = lax.axis_size(axis)
    return lax.ppermute(x, axis, [(i, i + by) for i in range(size) if 0 <= i + by < size])


def paired(matrix):
    rows, width = matrix.shape
    return matrix.reshape(rows, 2, -1, PAIR).transpose(0, 2, 1, 3).reshape(rows, width)


def unpaired(matrix):
    rows, width = matrix.shape
    return matrix.reshape(rows, -1, 2, PAIR).transpose(0, 2, 1, 3).reshape(rows, width)


def to_slabs(matrix, groups, slab):
    rows, columns = matrix.shape[0] // groups, matrix.shape[1]
    split = matrix.reshape(groups, rows, columns)
    pieces = [split[:, i * slab : (i + 1) * slab] for i in range(rows // slab)]
    rest = rows % slab
    if rest:
        tail = split[:, rows - rest :].reshape(groups, rest, slab // rest, columns * rest // slab)
        pieces.append(tail.transpose(0, 2, 1, 3).reshape(groups, slab, columns * rest // slab))
    return jnp.concatenate(pieces, axis=2).reshape(groups * slab, -1)


def from_slab(packed, shape):
    slab, (rows, columns) = packed.shape[0], shape
    whole, rest = divmod(rows, slab)
    pieces = [packed[:, i * columns : (i + 1) * columns] for i in range(whole)]
    if rest:
        tail = packed[:, whole * columns :].reshape(slab // rest, rest, columns * rest // slab)
        pieces.append(tail.transpose(1, 0, 2).reshape(rest, columns))
    return jnp.concatenate(pieces, axis=0)


def scattered(grads, axis):
    return lax.psum_scatter(grads.astype(BF16), axis, scatter_dimension=0, tiled=True)


def body(
    frames, text_states, timestep, frame_lengths, text_lengths,
    cond_weight, cond_bias, joint_weight, self_output, query_weight, text_weight, cross_output,
    up_weight, up_bias, down_weight, down_bias, cotangent,
):
    rows, width = frames.shape
    parts, position = lax.axis_size("text"), lax.axis_index("text")
    groups, group = lax.axis_size("seq"), lax.axis_index("seq")
    items, tokens, text_width = text_states.shape
    mod_width = cond_weight.shape[1]

    small = jnp.concatenate([timestep.reshape(-1), cond_bias, up_bias, down_bias]).astype(F32)
    small_all = lax.all_gather(small[None, :], "seq", axis=0)[:, 0]
    joint_local = jnp.concatenate([joint_weight[:, :width], paired(joint_weight[:, width:])], axis=1)
    joint_full = lax.all_gather(joint_local, "seq", axis=0, tiled=True)
    text_full = lax.all_gather(paired(text_weight), "seq", axis=0, tiled=True)
    outer_full = lax.all_gather(
        jnp.concatenate([self_output, query_weight, cross_output], axis=1), "seq", axis=0, tiled=True
    )
    up_full = lax.all_gather(up_weight, "seq", axis=0, tiled=True)
    down_full = lax.all_gather(down_weight, "seq", axis=0, tiled=True)
    before = neighbour(frames, "text", 1)
    after = neighbour(frames, "text", -1)
    flat_text = text_states.reshape(items * tokens, text_width)

    cut = timestep.size
    steps_all = small_all[:, :cut].reshape(groups * items, width)
    cond_bias_full = small_all[:, cut : cut + cond_bias.size].reshape(-1).astype(F32)
    cut += cond_bias.size
    up_bias_full = small_all[:, cut : cut + up_bias.size].reshape(-1).astype(F32)
    cut += up_bias.size
    down_bias_full = small_all[:, cut:].reshape(-1).astype(F32)

    silu_all = jax.nn.silu(steps_all.astype(F32)).astype(BF16)
    slab = cond_weight.shape[0]
    silu_mine = lax.dynamic_slice_in_dim(silu_all, group * slab, slab, axis=1)
    modulation = (
        lax.psum_scatter(product(silu_mine, cond_weight), "seq", scatter_dimension=0, tiled=True)
        + cond_bias_full
    )

    ends = jnp.cumsum(frame_lengths[0])
    starts = ends - frame_lengths[0]

    def item_of(places):
        inside = (places >= 0) & (places < rows * parts)
        found = jnp.sum((places[:, None] >= ends[None, :]).astype(jnp.int32), axis=1)
        return jnp.where(inside, found, -1)

    origin = (position - 1) * rows
    window_item = item_of(origin + jnp.arange(3 * rows, dtype=jnp.int32))
    own_item = window_item[rows : 2 * rows]
    token_index = jnp.arange(items * parts * tokens, dtype=jnp.int32)
    token_item = token_index // (parts * tokens)
    in_item = token_index % (parts * tokens)
    token_place = ((position - in_item // tokens) % parts) * tokens + in_item % tokens
    limits = jnp.broadcast_to(text_lengths[:, None], (items, parts * tokens)).reshape(-1)
    token_kind = jnp.where(token_place < limits, token_item, -1)
    query_tags, _ = tag_lanes(own_item, items)
    _, window_tags = tag_lanes(window_item, items)
    _, token_tags = tag_lanes(token_kind, items)
    firsts = own_item[:: BLOCK_Q]
    lasts = own_item[BLOCK_Q - 1 :: BLOCK_Q]
    self_bounds = jnp.stack(
        [(starts[firsts] - origin) // BLOCK_K, (ends[lasts] - origin + BLOCK_K - 1) // BLOCK_K]
    )
    per_text = parts * tokens // BLOCK_K
    cross_bounds = jnp.stack([firsts * per_text, (lasts + 1) * per_text])

    source = frames.astype(F32)
    window = (before, frames, after)
    select = selector(window_item)
    own = slice(rows, 2 * rows)
    blocks = [modulation[:, i * width : (i + 1) * width] for i in range(6)]
    scale_one, scale_two = exact_table(1.0 + blocks[1]), exact_table(1.0 + blocks[4])
    gate_one, gate_two = of_owner(own_item, blocks[2]), of_owner(own_item, blocks[5])
    normed_one, query, keyvalue = enter(
        window, select, exact_table(blocks[0]), scale_one, joint_full
    )
    late_text, query = lax.optimization_barrier((text_states, query))
    text_parts = [text_states] + [shifted(late_text, "text", k) for k in range(1, parts)]
    factor = HEAD_DIM ** (-0.5)
    mixed, self_lse = attend(2, self_bounds, query, keyvalue, query_tags, window_tags)
    mixed, text_parts = lax.optimization_barrier((mixed, text_parts))
    output_full = outer_full[:, :width]
    query_full = outer_full[:, width : 2 * width]
    cross_full = outer_full[:, 2 * width :]
    self_branch = product(mixed, output_full)
    after_self = source + gate_one * self_branch
    normed_two = layer_norm(after_self).astype(BF16)
    cross_query = product(normed_two, query_full).astype(BF16) * BF16(factor)
    text_all = jnp.concatenate(text_parts, axis=1).reshape(items * parts * tokens, text_width)
    text_kv = product(text_all, text_full).astype(BF16)
    cross_mixed, cross_lse = attend(
        1, cross_bounds, cross_query, text_kv, query_tags, token_tags
    )
    after_cross = after_self + product(cross_mixed, cross_full)
    normed_three = modulate(
        after_cross, of_owner(own_item, blocks[3]), of_owner(own_item, blocks[4])
    ).astype(BF16)
    hidden = product(normed_three, up_full) + up_bias_full
    activated = jax.nn.gelu(hidden, approximate=True).astype(BF16)
    mlp_branch = product(activated, down_full) + down_bias_full
    result = (after_cross + gate_two * mlp_branch).astype(BF16)

    upstream = cotangent.astype(F32)
    grad_branch = (gate_two * upstream).astype(BF16)
    grad_down = contract_first(activated, grad_branch).astype(BF16)
    grad_down_bias = jnp.sum(grad_branch.astype(F32), axis=0)
    grad_activated = contract_last(grad_branch, down_full)
    _, gelu_pull = jax.vjp(lambda entry: jax.nn.gelu(entry, approximate=True), hidden)
    grad_hidden = gelu_pull(grad_activated)[0].astype(BF16)
    grad_up = contract_first(normed_three, grad_hidden).astype(BF16)
    wide = jnp.concatenate([grad_up, to_slabs(grad_down, groups, slab)], axis=1)
    grad_up_bias = jnp.sum(grad_hidden.astype(F32), axis=0)
    grad_after_cross, sums_two = third(
        grad_hidden, up_full, after_cross, select[own], scale_two, cotangent, mlp_branch
    )
    grad_cross_branch = grad_after_cross.astype(BF16)
    grad_cross_mixed = contract_last(grad_cross_branch, cross_full).astype(BF16)
    grad_cross_mixed, wide = lax.optimization_barrier((grad_cross_mixed, wide))
    share_wide = scattered(wide, "seq")
    grad_cross_query, grad_text_kv = attend_back(
        1, cross_bounds, cross_query, text_kv, grad_cross_mixed, cross_mixed,
        query_tags, token_tags, cross_lse,
    )
    grad_text_weight = contract_first(text_all, grad_text_kv).astype(BF16)
    grad_text_all = contract_last(grad_text_kv, text_full).reshape(items, parts, tokens, text_width)
    grad_text = grad_text_all[:, 0]
    sent_text = [
        shifted(grad_text_all[:, k].astype(BF16), "text", -k) for k in range(1, parts)
    ]
    grad_normed_two = contract_last(grad_cross_query, query_full)
    _, norm_pull = jax.vjp(layer_norm, after_self)
    grad_after_self = grad_after_cross + norm_pull(grad_normed_two)[0]
    grad_self_branch = (gate_one * grad_after_self).astype(BF16)
    grad_self_branch, share_wide = lax.optimization_barrier((grad_self_branch, share_wide))
    summed_wide = lax.psum(share_wide, "text")
    mid = outer_grads(
        (mixed, normed_two, cross_mixed), (grad_self_branch, grad_cross_query, grad_cross_branch),
        to_slabs(grad_text_weight, groups, slab),
    )
    grad_mixed = contract_last(grad_self_branch, output_full).astype(BF16)
    grad_mixed, mid = lax.optimization_barrier((grad_mixed, mid))
    share_mid = scattered(mid, "seq")
    grad_query, grad_keyvalue = attend_back(
        2, self_bounds, query, keyvalue, grad_mixed, mixed, query_tags, window_tags, self_lse,
    )
    grad_query, sent_text, share_mid = lax.optimization_barrier((grad_query, sent_text, share_mid))
    for sent in sent_text:
        grad_text = grad_text + sent.astype(F32)
    joint = jnp.concatenate(
        [
            contract_first(normed_one[own], grad_query).astype(BF16),
            contract_first(normed_one, grad_keyvalue).astype(BF16),
        ],
        axis=1,
    )
    grad_query, grad_keyvalue, joint = lax.optimization_barrier((grad_query, grad_keyvalue, joint))
    share_joint = scattered(joint, "seq")
    grad_own, grad_halo, sums_one = leave(
        grad_query, grad_keyvalue, joint_full, window, select, scale_one, grad_after_self, self_branch
    )
    sums = jnp.concatenate(
        [part[slot * SLOTS : slot * SLOTS + items] for part in (sums_one, sums_two) for slot in range(3)],
        axis=1,
    )
    sums = jnp.concatenate([sums.reshape(-1), grad_up_bias, grad_down_bias])[None, :].astype(BF16)
    sums_all = lax.all_gather(lax.psum(sums, "text").astype(F32), "seq", axis=0)[:, 0]
    grad_halo, sums_all, summed_wide, share_mid, share_joint = lax.optimization_barrier(
        (grad_halo, sums_all, summed_wide, share_mid, share_joint)
    )
    from_next = neighbour(grad_halo[:rows], "text", -1)
    from_previous = neighbour(grad_halo[rows:], "text", 1)
    grad_frames = grad_own + from_next.astype(F32) + from_previous.astype(F32)
    summed_mid, summed_joint = lax.psum((share_mid, share_joint), "text")
    summed_joint = summed_joint.astype(F32)
    cut = items * mod_width
    grad_mod_all = sums_all[:, :cut].reshape(groups * items, mod_width)
    grad_cond_weight = lax.dot_general(
        silu_mine.astype(F32), grad_mod_all, (((0,), (0,)), ((), ())), precision=lax.Precision.HIGHEST
    )
    grad_cond_bias = jnp.sum(
        lax.dynamic_slice_in_dim(grad_mod_all, group * cond_bias.size, cond_bias.size, axis=1), axis=0
    )
    bias_sums = jnp.sum(sums_all[:, cut:], axis=0)
    share_up_bias = lax.dynamic_slice_in_dim(
        bias_sums[: up_bias.size * groups], group * up_bias.size, up_bias.size
    )
    share_down_bias = lax.dynamic_slice_in_dim(
        bias_sums[up_bias.size * groups :], group * down_bias.size, down_bias.size
    )
    summed_wide, summed_mid = summed_wide.astype(F32), summed_mid.astype(F32)
    up_width = up_weight.shape[1]
    return (
        result, grad_frames, grad_text, grad_cond_weight, grad_cond_bias,
        jnp.concatenate([summed_joint[:, :width], unpaired(summed_joint[:, width:])], axis=1),
        summed_mid[:, :width], summed_mid[:, width : 2 * width],
        unpaired(from_slab(summed_mid[:, 3 * width :], text_weight.shape)), summed_mid[:, 2 * width : 3 * width],
        summed_wide[:, :up_width], share_up_bias,
        from_slab(summed_wide[:, up_width:], down_weight.shape), share_down_bias,
    )


def solution(mesh):
    both, seq, flat = P(("seq", "text"), None), P("seq", None), P("seq")
    texts = P("seq", "text", None)
    return jax.shard_map(
        body,
        mesh=mesh,
        in_specs=(
            both, texts, seq, seq, flat, seq, flat, seq, seq, seq, seq, seq, seq, flat, seq, flat, both,
        ),
        out_specs=(
            both, both, texts, seq, flat, seq, seq, seq, seq, seq, seq, flat, seq, flat,
        ),
        check_vma=False,
    )
```

```python
import functools

import jax
import jax.numpy as jnp
from jax import lax
from jax.experimental import pallas as pl
from jax.experimental.pallas import tpu as pltpu
from jax.sharding import PartitionSpec as P

HEADS = 12
HEAD_DIM = 64
PAIR = 2 * HEAD_DIM
EPSILON = 1e-06
BLOCK_Q = 256
BLOCK_K = 256
PENALTY = -1e30
VMEM_LIMIT = 60 * 1024 * 1024

BF16 = jnp.bfloat16
F32 = jnp.float32


def contract(left, right, dims):
    return lax.dot_general(left, right, (dims, ((), ())), preferred_element_type=F32)


def product(left, right):
    return contract(left, right, ((1,), (0,)))


def contract_first(left, right):
    return contract(left, right, ((0,), (0,)))


def contract_last(left, right):
    return contract(left, right, ((1,), (1,)))


def halves():
    lane = lax.broadcasted_iota(jnp.int32, (1, PAIR), 1)
    low = (lane < HEAD_DIM).astype(F32).astype(BF16)
    return low, (lane >= HEAD_DIM).astype(F32).astype(BF16)


def rows_of(block, size):
    return pl.ds(pl.multiple_of(block * size, size), size)


def span(bounds, i, key_blocks, wide):
    first, last = bounds[0, i], bounds[1, i]
    steps = (last - first + wide - 1) // wide
    return jnp.minimum(first, key_blocks - wide * steps), steps


def forward_kernel(wide, bounds, q_ref, kv_ref, qt_ref, kt_ref, o_ref, lse_ref, ka_ref, vt_ref):
    low, high = halves()
    key_blocks = kv_ref.shape[0] // BLOCK_K
    ones = jnp.ones((16, BLOCK_K), F32).astype(BF16)

    @pl.loop(0, key_blocks)
    def _(b):
        rows = rows_of(b, BLOCK_K)
        keys, tags = kv_ref[rows, :PAIR], kt_ref[rows, :]
        ka_ref[0, rows, :] = keys * low + tags * high
        ka_ref[1, rows, :] = keys * high + tags * low
        turned = kv_ref[rows, PAIR:].astype(F32).T.astype(BF16)
        vt_ref[0, :HEAD_DIM, rows] = turned[:HEAD_DIM]
        vt_ref[1, :HEAD_DIM, rows] = turned[HEAD_DIM:]
        vt_ref[0, HEAD_DIM:, rows] = ones
        vt_ref[1, HEAD_DIM:, rows] = ones

    @pl.loop(0, q_ref.shape[0] // BLOCK_Q)
    def _(i):
        mine = rows_of(i, BLOCK_Q)
        queries, tags = q_ref[mine, :], qt_ref[mine, :]
        tagged = (queries * low + tags * high, queries * high + tags * low)
        first, steps = span(bounds, i, key_blocks, wide)

        def step(b, states):
            parts = [rows_of(first + wide * b + j, BLOCK_K) for j in range(wide)]
            scores = [[contract_last(ka_ref[h, rows, :], tagged[h]) for rows in parts] for h in range(2)]
            tops = []
            for h in range(2):
                top = states[h][0]
                for part in scores[h]:
                    top = jnp.maximum(top, jnp.max(part, axis=0, keepdims=True))
                tops.append(top)
            expos = [[jnp.exp(part - tops[h]).astype(BF16) for part in scores[h]] for h in range(2)]
            following = []
            for h in range(2):
                peak, acc = states[h]
                acc = acc * jnp.exp(peak - tops[h])
                for part, rows in zip(expos[h], parts):
                    acc = acc + product(vt_ref[h, :, rows], part)
                following.append((tops[h], acc))
            return tuple(following)

        start = (
            jnp.full((1, BLOCK_Q), 2 * PENALTY, F32),
            jnp.zeros((HEAD_DIM + 16, BLOCK_Q), F32),
        )
        ended = lax.fori_loop(0, steps, step, (start, start))
        totals = [acc[HEAD_DIM : HEAD_DIM + 1] for _, acc in ended]
        outs = [acc[:HEAD_DIM] / total for total, (_, acc) in zip(totals, ended)]
        o_ref[mine, :] = jnp.concatenate(outs, axis=0).T.astype(BF16)
        for h in range(2):
            lse_ref[0, h : h + 1, mine] = ended[h][0] + jnp.log(totals[h])


def backward_kernel(
    wide, bounds, q_ref, kv_ref, g_ref, o_ref, qt_ref, kt_ref, lse_ref,
    dq_ref, dkv_ref, ka_ref, kt_s, dqt, dk_acc, dv_acc,
):
    low, high = halves()
    key_blocks = kv_ref.shape[0] // BLOCK_K

    @pl.loop(0, key_blocks)
    def _(b):
        rows = rows_of(b, BLOCK_K)
        keys, tags = kv_ref[rows, :PAIR], kt_ref[rows, :]
        ka_ref[0, rows, :] = keys * low + tags * high
        ka_ref[1, rows, :] = keys * high + tags * low
        kt_s[:, rows] = keys.astype(F32).T.astype(BF16)
        dk_acc[:, rows] = jnp.zeros((PAIR, BLOCK_K), F32)
        dv_acc[:, rows] = jnp.zeros((PAIR, BLOCK_K), F32)

    @pl.loop(0, q_ref.shape[0] // BLOCK_Q)
    def _(i):
        mine = rows_of(i, BLOCK_Q)
        queries, tags, grads = q_ref[mine, :], qt_ref[mine, :], g_ref[mine, :]
        tagged = (queries * low + tags * high, queries * high + tags * low)
        split = (grads * low, grads * high)
        q_turned = queries.astype(F32).T.astype(BF16)
        g_turned = grads.astype(F32).T
        pulls = g_turned * o_ref[mine, :].astype(F32).T
        deltas = [jnp.sum(pulls[:HEAD_DIM], axis=0, keepdims=True)]
        deltas.append(jnp.sum(pulls[HEAD_DIM:], axis=0, keepdims=True))
        g_turned = g_turned.astype(BF16)
        lses = [lse_ref[0, h : h + 1, mine] for h in range(2)]
        dqt[...] = jnp.zeros(dqt.shape, F32)
        first, steps = span(bounds, i, key_blocks, wide)

        @pl.loop(0, steps)
        def _(b):
            found = []
            for j in range(wide):
                rows = rows_of(first + wide * b + j, BLOCK_K)
                for h in range(2):
                    scores = contract_last(ka_ref[h, rows, :], tagged[h])
                    found.append((h, rows, scores, contract_last(kv_ref[rows, PAIR:], split[h])))
            made = []
            for h, rows, scores, pull in found:
                expos = jnp.exp(scores - lses[h])
                slope = (expos * (pull - deltas[h])).astype(BF16)
                made.append((h, rows, expos.astype(BF16), slope))
            for h, rows, weight, slope in made:
                part = slice(h * HEAD_DIM, (h + 1) * HEAD_DIM)
                dk_acc[part, rows] += contract_last(q_turned[part], slope)
                dv_acc[part, rows] += contract_last(g_turned[part], weight)
                dqt[part, :] += product(kt_s[part, rows], slope)

        dq_ref[mine, :] = (dqt[...] * HEAD_DIM ** (-0.5)).T.astype(BF16)

    @pl.loop(0, key_blocks)
    def _(b):
        rows = rows_of(b, BLOCK_K)
        dkv_ref[rows, :PAIR] = dk_acc[:, rows].T.astype(BF16)
        dkv_ref[rows, PAIR:] = dv_acc[:, rows].T.astype(BF16)


def column(rows):
    return pl.BlockSpec((rows, PAIR), lambda j, *_: (0, j))


def double(rows):
    return pl.BlockSpec((rows, 2 * PAIR), lambda j, *_: (0, j))


def shared(rows):
    return pl.BlockSpec((rows, PAIR), lambda j, *_: (0, 0))


def stat(rows):
    return pl.BlockSpec((1, 8, rows), lambda j, *_: (j, 0, 0))


def cost(rows, keys, matmuls):
    return pl.CostEstimate(
        flops=matmuls * rows * keys * HEADS * HEAD_DIM, bytes_accessed=8 * (rows + keys) * HEADS * HEAD_DIM,
        transcendentals=rows * keys * HEADS // 2,
    )


def attend(wide, bounds, query, keyvalue, query_tags, key_tags):
    rows, width = query.shape
    keys = keyvalue.shape[0]
    return pl.pallas_call(
        functools.partial(forward_kernel, wide),
        out_shape=(
            jax.ShapeDtypeStruct((rows, width), BF16),
            jax.ShapeDtypeStruct((width // PAIR, 8, rows), F32),
        ),
        grid_spec=pltpu.PrefetchScalarGridSpec(
            num_scalar_prefetch=1,
            grid=(width // PAIR,),
            in_specs=[column(rows), double(keys), shared(rows), shared(keys)],
            out_specs=[column(rows), stat(rows)],
            scratch_shapes=[
                pltpu.VMEM((2, keys, PAIR), BF16),
                pltpu.VMEM((2, HEAD_DIM + 16, keys), BF16),
            ],
        ),
        compiler_params=pltpu.CompilerParams(vmem_limit_bytes=VMEM_LIMIT),
        cost_estimate=cost(rows, keys, 4),
        name="attend",
    )(bounds, query, keyvalue, query_tags, key_tags)


def attend_back(wide, bounds, query, keyvalue, grad, out, query_tags, key_tags, lse):
    rows, width = query.shape
    keys = keyvalue.shape[0]
    return pl.pallas_call(
        functools.partial(backward_kernel, wide),
        out_shape=(
            jax.ShapeDtypeStruct((rows, width), BF16),
            jax.ShapeDtypeStruct((keys, 2 * width), BF16),
        ),
        grid_spec=pltpu.PrefetchScalarGridSpec(
            num_scalar_prefetch=1,
            grid=(width // PAIR,),
            in_specs=[
                column(rows), double(keys), column(rows), column(rows), shared(rows), shared(keys),
                stat(rows),
            ],
            out_specs=[column(rows), double(keys)],
            scratch_shapes=[
                pltpu.VMEM((2, keys, PAIR), BF16),
                pltpu.VMEM((PAIR, keys), BF16),
                pltpu.VMEM((PAIR, BLOCK_Q), F32),
                pltpu.VMEM((PAIR, keys), F32),
                pltpu.VMEM((PAIR, keys), F32),
            ],
        ),
        compiler_params=pltpu.CompilerParams(vmem_limit_bytes=VMEM_LIMIT),
        cost_estimate=cost(rows, keys, 10),
        name="attend_back",
    )(bounds, query, keyvalue, grad, out, query_tags, key_tags, lse)


TILE = 256
COPIES = 3
SLOTS = 8


def normed(values):
    centre = values - jnp.mean(values, axis=-1, keepdims=True)
    scale = lax.rsqrt(jnp.mean(centre * centre, axis=-1, keepdims=True) + EPSILON)
    return centre * scale, scale


def take(tile, own, before_ref, frames_ref, after_ref, x_ref):
    inside = (tile >= own[0]) & (tile < own[1])
    for chosen, ref in ((tile < own[0], before_ref), (inside, frames_ref), (tile >= own[1], after_ref)):

        @pl.when(chosen)
        def _(ref=ref):
            x_ref[...] = ref[...].astype(F32)


def window_tiles(width, first, last):
    def at(start, count):
        return tiles(width, lambda t: jnp.clip(t - start, 0, count - 1))

    return [at(0, first), at(first, last - first), at(last, first)]


def enter_kernel(own, before_ref, frames_ref, after_ref, sel_ref, shift_ref, scale_ref, w_ref, h_ref, q_ref, kv_ref, x_ref):
    tile = pl.program_id(0)
    width = x_ref.shape[1]
    take(tile, own, before_ref, frames_ref, after_ref, x_ref)
    norm, _ = normed(x_ref[...])
    select = sel_ref[...]
    values = norm * product(select, scale_ref[...]) + product(select, shift_ref[...])
    values = values.astype(BF16)
    h_ref[...] = values
    kv_ref[...] = product(values, w_ref[:, width:]).astype(BF16)

    @pl.when((tile >= own[0]) & (tile < own[1]))
    def _():
        q_ref[...] = (product(values, w_ref[:, :width]) * HEAD_DIM ** (-0.5)).astype(BF16)


def leave_kernel(
    own, dq_ref, dkv_ref, w_ref, before_ref, frames_ref, after_ref, sel_ref, scale_ref, add_ref, branch_ref,
    own_ref, halo_ref, sums_ref, gh_ref, x_ref,
):
    tile = pl.program_id(0)
    width = x_ref.shape[1]
    mine = (tile >= own[0]) & (tile < own[1])

    @pl.when(tile == 0)
    def _():
        sums_ref[...] = jnp.zeros(sums_ref.shape, F32)

    gh_ref[...] = contract_last(dkv_ref[...], w_ref[:, width:])

    @pl.when(mine)
    def _():
        gh_ref[...] += contract_last(dq_ref[...], w_ref[:, :width])

    take(tile, own, before_ref, frames_ref, after_ref, x_ref)
    grad = gh_ref[...]
    norm, scale = normed(x_ref[...])
    select = sel_ref[...]
    add_sums(sums_ref, select, grad, grad * norm)
    moved = grad * product(select, scale_ref[...])
    moved = norm_back(moved, norm, scale)

    @pl.when(mine)
    def _():
        own_ref[...] = moved + add_ref[...]
        add_sums(sums_ref, select, add_ref[...] * branch_ref[...], at=2)

    @pl.when(jnp.logical_not(mine))
    def _():
        halo_ref[...] = moved.astype(BF16)


def norm_back(grad, norm, scale):
    inner = jnp.mean(grad * norm, axis=-1, keepdims=True)
    return scale * (grad - jnp.mean(grad, axis=-1, keepdims=True) - norm * inner)


def add_sums(sums_ref, select, *terms, at=0):
    for slot, values in enumerate(terms, at):
        coarse = values.astype(BF16)
        fine = (values - coarse.astype(F32)).astype(BF16)
        total = contract_first(select, coarse) + contract_first(select, fine)
        sums_ref[slot * SLOTS : (slot + 1) * SLOTS, :] += total[:SLOTS]


def third_kernel(g_ref, w_ref, x_ref, sel_ref, scale_ref, add_ref, branch_ref, out_ref, round_ref, sums_ref):
    @pl.when(pl.program_id(0) == 0)
    def _():
        sums_ref[...] = jnp.zeros(sums_ref.shape, F32)

    grad = contract_last(g_ref[...], w_ref[...])
    norm, scale = normed(x_ref[...])
    select = sel_ref[...]
    addend = add_ref[...].astype(F32)
    add_sums(sums_ref, select, grad, grad * norm, addend * branch_ref[...])
    moved = grad * product(select, scale_ref[...])
    total = norm_back(moved, norm, scale) + addend
    out_ref[...] = total
    round_ref[...] = total.astype(BF16)


def tiles(width, at=lambda t: t):
    return pl.BlockSpec((TILE, width), lambda t: (at(t), 0))


def whole(array):
    return pl.BlockSpec(array.shape, lambda t: (0, 0), pipeline_mode=pl.Buffered(1))


def enter(window, select, shift, scale, weight):
    rows, width = window[1].shape
    count = 3 * rows
    first, last = rows // TILE, 2 * rows // TILE
    return pl.pallas_call(
        functools.partial(enter_kernel, (first, last)),
        grid=(count // TILE,),
        out_shape=(
            jax.ShapeDtypeStruct((count, width), BF16),
            jax.ShapeDtypeStruct((rows, width), BF16),
            jax.ShapeDtypeStruct((count, 2 * width), BF16),
        ),
        in_specs=[
            *window_tiles(width, first, last), tiles(PAIR), whole(shift), whole(scale), whole(weight),
        ],
        out_specs=[
            tiles(width), tiles(width, lambda t: jnp.clip(t - first, 0, last - first - 1)), tiles(2 * width),
        ],
        scratch_shapes=[pltpu.VMEM((TILE, width), F32)],
        compiler_params=pltpu.CompilerParams(vmem_limit_bytes=VMEM_LIMIT),
        cost_estimate=pl.CostEstimate(
            flops=6 * count * width * width, bytes_accessed=8 * count * width, transcendentals=0
        ),
        name="enter",
    )(*window, select, shift, scale, weight)


def leave(grad_query, grad_keyvalue, weight, window, select, scale, addend, branch):
    rows, width = grad_query.shape
    count = 3 * rows
    first, last = rows // TILE, 2 * rows // TILE

    def own(t):
        return jnp.clip(t - first, 0, last - first - 1)

    def halo(t):
        return jnp.where(t < first, t, jnp.maximum(t - (last - first), first - 1))

    return pl.pallas_call(
        functools.partial(leave_kernel, (first, last)),
        grid=(count // TILE,),
        out_shape=(
            jax.ShapeDtypeStruct((rows, width), F32),
            jax.ShapeDtypeStruct((count - rows, width), BF16),
            jax.ShapeDtypeStruct((3 * SLOTS, width), F32),
        ),
        in_specs=[
            tiles(width, own), tiles(2 * width), whole(weight), *window_tiles(width, first, last),
            tiles(PAIR), whole(scale), tiles(width, own), tiles(width, own),
        ],
        out_specs=[
            tiles(width, own), tiles(width, halo), pl.BlockSpec((3 * SLOTS, width), lambda t: (0, 0)),
        ],
        scratch_shapes=[pltpu.VMEM((TILE, width), F32), pltpu.VMEM((TILE, width), F32)],
        compiler_params=pltpu.CompilerParams(vmem_limit_bytes=VMEM_LIMIT),
        cost_estimate=pl.CostEstimate(
            flops=6 * count * width * width, bytes_accessed=8 * count * width, transcendentals=0
        ),
        name="leave",
    )(grad_query, grad_keyvalue, weight, *window, select, scale, addend, branch)


def third(grad, weight, values, select, scale, addend, branch):
    rows, width = values.shape
    return pl.pallas_call(
        third_kernel,
        grid=(rows // TILE,),
        out_shape=(
            jax.ShapeDtypeStruct((rows, width), F32),
            jax.ShapeDtypeStruct((rows, width), BF16),
            jax.ShapeDtypeStruct((3 * SLOTS, width), F32),
        ),
        in_specs=[
            tiles(grad.shape[1]), whole(weight), tiles(width), tiles(PAIR), whole(scale), tiles(width),
            tiles(width),
        ],
        out_specs=[tiles(width), tiles(width), pl.BlockSpec((3 * SLOTS, width), lambda t: (0, 0))],
        compiler_params=pltpu.CompilerParams(vmem_limit_bytes=VMEM_LIMIT),
        cost_estimate=pl.CostEstimate(
            flops=2 * rows * width * grad.shape[1], bytes_accessed=16 * rows * width, transcendentals=0
        ),
        name="third",
    )(grad, weight, values, select, scale, addend, branch)


def outer_kernel(*refs):
    lefts, rights, slab_ref, out_ref, acc_ref = refs[:3], refs[3:6], refs[6], refs[7], refs[8]
    width = lefts[0].shape[1]

    @pl.when(pl.program_id(0) == 0)
    def _():
        acc_ref[...] = jnp.zeros(acc_ref.shape, F32)

    for i, (left, right) in enumerate(zip(lefts, rights)):
        acc_ref[:, i * width : (i + 1) * width] += contract_first(left[...], right[...])

    @pl.when(pl.program_id(0) == pl.num_programs(0) - 1)
    def _():
        out_ref[:, : 3 * width] = acc_ref[...].astype(BF16)
        out_ref[:, 3 * width :] = slab_ref[...]


def outer_grads(lefts, rights, slab):
    rows, width = lefts[0].shape
    shape = (width, 3 * width + slab.shape[1])
    return pl.pallas_call(
        outer_kernel,
        grid=(rows // TILE,),
        out_shape=jax.ShapeDtypeStruct(shape, BF16),
        in_specs=[tiles(width)] * 6 + [whole(slab)],
        out_specs=pl.BlockSpec(shape, lambda t: (0, 0)),
        scratch_shapes=[pltpu.VMEM((width, 3 * width), F32)],
        compiler_params=pltpu.CompilerParams(vmem_limit_bytes=VMEM_LIMIT),
        cost_estimate=pl.CostEstimate(
            flops=6 * rows * width * width, bytes_accessed=12 * rows * width + 4 * shape[0] * shape[1],
            transcendentals=0,
        ),
        name="outer_grads",
    )(*lefts, *rights, slab)


def selector(owner):
    lane = jnp.arange(PAIR, dtype=jnp.int32)[None, :]
    return ((lane < COPIES * SLOTS) & (lane % SLOTS == owner[:, None])).astype(BF16)


def exact_table(table):
    left = jnp.pad(table, ((0, SLOTS - table.shape[0]), (0, 0)))
    pieces = []
    for _ in range(COPIES):
        pieces.append(lax.reduce_precision(left, 8, 7))
        left = left - pieces[-1]
    return jnp.pad(jnp.concatenate(pieces, axis=0), ((0, PAIR - COPIES * SLOTS), (0, 0))).astype(BF16)


def tag_lanes(kind, items):
    lane = jnp.arange(PAIR, dtype=jnp.int32)[None, :] % HEAD_DIM
    kind = jnp.where(kind < 0, items, kind)[:, None]
    key_tags = (lane == kind).astype(BF16)
    query_tags = jnp.where((lane != kind) & (lane <= items), PENALTY, 0.0).astype(BF16)
    return query_tags, key_tags


def layer_norm(values):
    centre = values - jnp.mean(values, axis=-1, keepdims=True)
    return centre * lax.rsqrt(jnp.mean(centre * centre, axis=-1, keepdims=True) + EPSILON)


def modulate(values, shift, scale):
    return layer_norm(values) * (1.0 + scale) + shift


def of_owner(owner, table):
    chosen = jnp.broadcast_to(table[0][None, :], (owner.shape[0], table.shape[1]))
    for item in range(1, table.shape[0]):
        chosen = jnp.where((owner == item)[:, None], table[item][None, :], chosen)
    return chosen


def shifted(x, axis, by):
    size = lax.axis_size(axis)
    return lax.ppermute(x, axis, [(i, (i + by) % size) for i in range(size)])


def neighbour(x, axis, by):
    size = lax.axis_size(axis)
    return lax.ppermute(x, axis, [(i, i + by) for i in range(size) if 0 <= i + by < size])


def paired(matrix):
    rows, width = matrix.shape
    return matrix.reshape(rows, 2, -1, PAIR).transpose(0, 2, 1, 3).reshape(rows, width)


def unpaired(matrix):
    rows, width = matrix.shape
    return matrix.reshape(rows, -1, 2, PAIR).transpose(0, 2, 1, 3).reshape(rows, width)


def to_slabs(matrix, groups, slab):
    rows, columns = matrix.shape[0] // groups, matrix.shape[1]
    split = matrix.reshape(groups, rows, columns)
    pieces = [split[:, i * slab : (i + 1) * slab] for i in range(rows // slab)]
    rest = rows % slab
    if rest:
        tail = split[:, rows - rest :].reshape(groups, rest, slab // rest, columns * rest // slab)
        pieces.append(tail.transpose(0, 2, 1, 3).reshape(groups, slab, columns * rest // slab))
    return jnp.concatenate(pieces, axis=2).reshape(groups * slab, -1)


def from_slab(packed, shape):
    slab, (rows, columns) = packed.shape[0], shape
    whole, rest = divmod(rows, slab)
    pieces = [packed[:, i * columns : (i + 1) * columns] for i in range(whole)]
    if rest:
        tail = packed[:, whole * columns :].reshape(slab // rest, rest, columns * rest // slab)
        pieces.append(tail.transpose(1, 0, 2).reshape(rest, columns))
    return jnp.concatenate(pieces, axis=0)


def scattered(grads, axis):
    return lax.psum_scatter(grads.astype(BF16), axis, scatter_dimension=0, tiled=True)


def body(
    frames, text_states, timestep, frame_lengths, text_lengths,
    cond_weight, cond_bias, joint_weight, self_output, query_weight, text_weight, cross_output,
    up_weight, up_bias, down_weight, down_bias, cotangent,
):
    rows, width = frames.shape
    parts, position = lax.axis_size("text"), lax.axis_index("text")
    groups, group = lax.axis_size("seq"), lax.axis_index("seq")
    items, tokens, text_width = text_states.shape
    mod_width = cond_weight.shape[1]

    small = jnp.concatenate([timestep.reshape(-1), cond_bias, up_bias, down_bias]).astype(F32)
    small_all = lax.all_gather(small[None, :], "seq", axis=0)[:, 0]
    joint_local = jnp.concatenate([joint_weight[:, :width], paired(joint_weight[:, width:])], axis=1)
    joint_full = lax.all_gather(joint_local, "seq", axis=0, tiled=True)
    text_full = lax.all_gather(paired(text_weight), "seq", axis=0, tiled=True)
    outer_full = lax.all_gather(
        jnp.concatenate([self_output, query_weight, cross_output], axis=1), "seq", axis=0, tiled=True
    )
    up_full = lax.all_gather(up_weight, "seq", axis=0, tiled=True)
    down_full = lax.all_gather(down_weight, "seq", axis=0, tiled=True)
    before = neighbour(frames, "text", 1)
    after = neighbour(frames, "text", -1)
    flat_text = text_states.reshape(items * tokens, text_width)

    cut = timestep.size
    steps_all = small_all[:, :cut].reshape(groups * items, width)
    cond_bias_full = small_all[:, cut : cut + cond_bias.size].reshape(-1).astype(F32)
    cut += cond_bias.size
    up_bias_full = small_all[:, cut : cut + up_bias.size].reshape(-1).astype(F32)
    cut += up_bias.size
    down_bias_full = small_all[:, cut:].reshape(-1).astype(F32)

    silu_all = jax.nn.silu(steps_all.astype(F32)).astype(BF16)
    slab = cond_weight.shape[0]
    silu_mine = lax.dynamic_slice_in_dim(silu_all, group * slab, slab, axis=1)
    modulation = (
        lax.psum_scatter(product(silu_mine, cond_weight), "seq", scatter_dimension=0, tiled=True)
        + cond_bias_full
    )

    ends = jnp.cumsum(frame_lengths[0])
    starts = ends - frame_lengths[0]

    def item_of(places):
        inside = (places >= 0) & (places < rows * parts)
        found = jnp.sum((places[:, None] >= ends[None, :]).astype(jnp.int32), axis=1)
        return jnp.where(inside, found, -1)

    origin = (position - 1) * rows
    window_item = item_of(origin + jnp.arange(3 * rows, dtype=jnp.int32))
    own_item = window_item[rows : 2 * rows]
    token_index = jnp.arange(items * parts * tokens, dtype=jnp.int32)
    token_item = token_index // (parts * tokens)
    in_item = token_index % (parts * tokens)
    token_place = ((position - in_item // tokens) % parts) * tokens + in_item % tokens
    limits = jnp.broadcast_to(text_lengths[:, None], (items, parts * tokens)).reshape(-1)
    token_kind = jnp.where(token_place < limits, token_item, -1)
    query_tags, _ = tag_lanes(own_item, items)
    _, window_tags = tag_lanes(window_item, items)
    _, token_tags = tag_lanes(token_kind, items)
    firsts = own_item[:: BLOCK_Q]
    lasts = own_item[BLOCK_Q - 1 :: BLOCK_Q]
    self_bounds = jnp.stack(
        [(starts[firsts] - origin) // BLOCK_K, (ends[lasts] - origin + BLOCK_K - 1) // BLOCK_K]
    )
    per_text = parts * tokens // BLOCK_K
    cross_bounds = jnp.stack([firsts * per_text, (lasts + 1) * per_text])

    source = frames.astype(F32)
    window = (before, frames, after)
    select = selector(window_item)
    own = slice(rows, 2 * rows)
    blocks = [modulation[:, i * width : (i + 1) * width] for i in range(6)]
    scale_one, scale_two = exact_table(1.0 + blocks[1]), exact_table(1.0 + blocks[4])
    gate_one, gate_two = of_owner(own_item, blocks[2]), of_owner(own_item, blocks[5])
    normed_one, query, keyvalue = enter(
        window, select, exact_table(blocks[0]), scale_one, joint_full
    )
    late_text, query = lax.optimization_barrier((text_states, query))
    text_parts = [text_states] + [shifted(late_text, "text", k) for k in range(1, parts)]
    factor = HEAD_DIM ** (-0.5)
    mixed, self_lse = attend(2, self_bounds, query, keyvalue, query_tags, window_tags)
    output_full = outer_full[:, :width]
    query_full = outer_full[:, width : 2 * width]
    cross_full = outer_full[:, 2 * width :]
    self_branch = product(mixed, output_full)
    after_self = source + gate_one * self_branch
    normed_two = layer_norm(after_self).astype(BF16)
    cross_query = product(normed_two, query_full).astype(BF16) * BF16(factor)
    cross_query, text_parts = lax.optimization_barrier((cross_query, text_parts))
    text_all = jnp.concatenate(text_parts, axis=1).reshape(items * parts * tokens, text_width)
    text_kv = product(text_all, text_full).astype(BF16)
    cross_mixed, cross_lse = attend(
        1, cross_bounds, cross_query, text_kv, query_tags, token_tags
    )
    after_cross = after_self + product(cross_mixed, cross_full)
    normed_three = modulate(
        after_cross, of_owner(own_item, blocks[3]), of_owner(own_item, blocks[4])
    ).astype(BF16)
    hidden = product(normed_three, up_full) + up_bias_full
    activated = jax.nn.gelu(hidden, approximate=True).astype(BF16)
    mlp_branch = product(activated, down_full) + down_bias_full
    result = (after_cross + gate_two * mlp_branch).astype(BF16)

    upstream = cotangent.astype(F32)
    grad_branch = (gate_two * upstream).astype(BF16)
    grad_down = contract_first(activated, grad_branch).astype(BF16)
    grad_down_bias = jnp.sum(grad_branch.astype(F32), axis=0)
    grad_activated = contract_last(grad_branch, down_full)
    _, gelu_pull = jax.vjp(lambda entry: jax.nn.gelu(entry, approximate=True), hidden)
    grad_hidden = gelu_pull(grad_activated)[0].astype(BF16)
    grad_up = contract_first(normed_three, grad_hidden).astype(BF16)
    wide = jnp.concatenate([grad_up, to_slabs(grad_down, groups, slab)], axis=1)
    grad_up_bias = jnp.sum(grad_hidden.astype(F32), axis=0)
    grad_after_cross, grad_cross_branch, sums_two = third(
        grad_hidden, up_full, after_cross, select[own], scale_two, cotangent, mlp_branch
    )
    grad_cross_mixed = contract_last(grad_cross_branch, cross_full).astype(BF16)
    grad_cross_mixed, wide = lax.optimization_barrier((grad_cross_mixed, wide))
    share_wide = scattered(wide, "seq")
    grad_cross_query, grad_text_kv = attend_back(
        1, cross_bounds, cross_query, text_kv, grad_cross_mixed, cross_mixed,
        query_tags, token_tags, cross_lse,
    )
    grad_text_weight = contract_first(text_all, grad_text_kv).astype(BF16)
    grad_text_all = contract_last(grad_text_kv, text_full).reshape(items, parts, tokens, text_width)
    grad_text = grad_text_all[:, 0]
    sent_text = [
        shifted(grad_text_all[:, k].astype(BF16), "text", -k) for k in range(1, parts)
    ]
    grad_normed_two = contract_last(grad_cross_query, query_full)
    _, norm_pull = jax.vjp(layer_norm, after_self)
    grad_after_self = grad_after_cross + norm_pull(grad_normed_two)[0]
    grad_self_branch = (gate_one * grad_after_self).astype(BF16)
    mid = outer_grads(
        (mixed, normed_two, cross_mixed), (grad_self_branch, grad_cross_query, grad_cross_branch),
        to_slabs(grad_text_weight, groups, slab),
    )
    grad_mixed = contract_last(grad_self_branch, output_full).astype(BF16)
    grad_mixed, mid, share_wide = lax.optimization_barrier((grad_mixed, mid, share_wide))
    share_mid = scattered(mid, "seq")
    summed_wide = lax.psum(share_wide, "text")
    grad_query, grad_keyvalue = attend_back(
        2, self_bounds, query, keyvalue, grad_mixed, mixed, query_tags, window_tags, self_lse,
    )
    grad_query, sent_text, share_mid = lax.optimization_barrier((grad_query, sent_text, share_mid))
    for sent in sent_text:
        grad_text = grad_text + sent.astype(F32)
    joint = jnp.concatenate(
        [
            contract_first(normed_one[own], grad_query).astype(BF16),
            contract_first(normed_one, grad_keyvalue).astype(BF16),
        ],
        axis=1,
    )
    grad_query, grad_keyvalue, joint = lax.optimization_barrier((grad_query, grad_keyvalue, joint))
    share_joint = scattered(joint, "seq")
    grad_own, grad_halo, sums_one = leave(
        grad_query, grad_keyvalue, joint_full, window, select, scale_one, grad_after_self, self_branch
    )
    sums = jnp.concatenate(
        [part[slot * SLOTS : slot * SLOTS + items] for part in (sums_one, sums_two) for slot in range(3)],
        axis=1,
    )
    sums = jnp.concatenate([sums.reshape(-1), grad_up_bias, grad_down_bias])[None, :].astype(BF16)
    sums_all = lax.all_gather(lax.psum(sums, "text").astype(F32), "seq", axis=0)[:, 0]
    from_next = neighbour(grad_halo[:rows], "text", -1)
    from_previous = neighbour(grad_halo[rows:], "text", 1)
    share_joint, share_mid, summed_wide, sums_all, from_next, from_previous = lax.optimization_barrier(
        (share_joint, share_mid, summed_wide, sums_all, from_next, from_previous)
    )
    grad_frames = grad_own + from_next.astype(F32) + from_previous.astype(F32)
    summed_mid, summed_joint = lax.psum((share_mid, share_joint), "text")
    summed_joint = summed_joint.astype(F32)
    cut = items * mod_width
    grad_mod_all = sums_all[:, :cut].reshape(groups * items, mod_width)
    grad_cond_weight = lax.dot_general(
        silu_mine.astype(F32), grad_mod_all, (((0,), (0,)), ((), ())), precision=lax.Precision.HIGHEST
    )
    grad_cond_bias = jnp.sum(
        lax.dynamic_slice_in_dim(grad_mod_all, group * cond_bias.size, cond_bias.size, axis=1), axis=0
    )
    bias_sums = jnp.sum(sums_all[:, cut:], axis=0)
    share_up_bias = lax.dynamic_slice_in_dim(
        bias_sums[: up_bias.size * groups], group * up_bias.size, up_bias.size
    )
    share_down_bias = lax.dynamic_slice_in_dim(
        bias_sums[up_bias.size * groups :], group * down_bias.size, down_bias.size
    )
    summed_wide, summed_mid = summed_wide.astype(F32), summed_mid.astype(F32)
    up_width = up_weight.shape[1]
    return (
        result, grad_frames, grad_text, grad_cond_weight, grad_cond_bias,
        jnp.concatenate([summed_joint[:, :width], unpaired(summed_joint[:, width:])], axis=1),
        summed_mid[:, :width], summed_mid[:, width : 2 * width],
        unpaired(from_slab(summed_mid[:, 3 * width :], text_weight.shape)), summed_mid[:, 2 * width : 3 * width],
        summed_wide[:, :up_width], share_up_bias,
        from_slab(summed_wide[:, up_width:], down_weight.shape), share_down_bias,
    )


def solution(mesh):
    both, seq, flat = P(("seq", "text"), None), P("seq", None), P("seq")
    texts = P("seq", "text", None)
    return jax.shard_map(
        body,
        mesh=mesh,
        in_specs=(
            both, texts, seq, seq, flat, seq, flat, seq, seq, seq, seq, seq, seq, flat, seq, flat, both,
        ),
        out_specs=(
            both, both, texts, seq, flat, seq, seq, seq, seq, seq, seq, flat, seq, flat,
        ),
        check_vma=False,
    )
```
